32 devices in a mesh: group: 2 (over x), fsdp: 4 (over z), inner: 4 (over y, core).
Axes of the slice: x: 2, y: 2, z: 4, core: 2. Of those that a mesh axis runs over, the one named last changes fastest.
Arguments:
- query_latent: bfloat16 [64, 3, 1536], P(('group', 'inner')), may hold values from -12 to 12
- new_entries: bfloat16 [64, 3, 576], P(('group', 'inner')), may hold values from -6 to 6
- latent_cache: bfloat16 [64, 512, 576], P(('group', 'inner')), may hold values from -800 to 800
- lengths: int32 [64], P(('group', 'inner')), may hold values from 128 to 512
- query_up: float32 [1536, 1024], P(('group', 'inner'), 'fsdp'), may hold values from -0.15625 to 0.15625
- key_up: float32 [512, 1024], P(('group', 'inner'), 'fsdp'), may hold values from -0.25 to 0.25
- query_moment: float32 [1536, 1024], P(('group', 'inner'), 'fsdp'), may hold values from -3 to 3
- query_second: float32 [1536, 1024], P(('group', 'inner'), 'fsdp'), may hold values from 0.05 to 2
- key_moment: float32 [512, 1024], P(('group', 'inner'), 'fsdp'), may hold values from -3 to 3
- key_second: float32 [512, 1024], P(('group', 'inner'), 'fsdp'), may hold values from 0.05 to 2
- query_grads: bfloat16 [12288, 1024], P(('group', 'inner'), 'fsdp'), may hold values from -6 to 6
- key_grads: bfloat16 [4096, 1024], P(('group', 'inner'), 'fsdp'), may hold values from -6 to 6
- rope_query: bfloat16 [1536, 512], P(None, 'fsdp'), may hold values from -0.15625 to 0.15625
- value_up: bfloat16 [512, 1024], P(None, 'fsdp'), may hold values from -0.25 to 0.25
- output_weight: bfloat16 [1024, 7168], P('fsdp'), may hold values from -0.25 to 0.25
Outputs:
- query_weight: float32 [1536, 1024], P(('group', 'inner'), 'fsdp')
- key_weight: float32 [512, 1024], P(('group', 'inner'), 'fsdp')
- query_first: float32 [1536, 1024], P(('group', 'inner'), 'fsdp')
- query_square: float32 [1536, 1024], P(('group', 'inner'), 'fsdp')
- key_first: float32 [512, 1024], P(('group', 'inner'), 'fsdp')
- key_square: float32 [512, 1024], P(('group', 'inner'), 'fsdp')
- attended: bfloat16 [7168, 192], P('fsdp', ('group', 'inner'))
The draws below stay inside these ranges and needn't reach their ends.
Inputs may be any that keep to these rules, and one draw needn't show every extreme that they name: `lengths`: each row's count of live cache slots; the new tokens follow them.
All inputs are finite; a program needn't handle non-finite values.
Results may differ from the reference program's by a relative error of at most 0.023.
Values may be sent and summed in bfloat16 or wider, within the bound.
No kernel may reach another device: no remote copies, remote signals or barrier semaphores. Data moves between devices by JAX's collectives and lax.ppermute only.
A program may use at most 64 MiB of HBM per device.

```python
import math
import jax
import jax.numpy as jnp
from jax import lax

D = 7168
QR = 1536
KL = 512
HD = 128
R = 64
STEPS = 3
CACHE = 512
H = 8
ROWS = 64
N_GROUP = 2
N_INNER = 4


def draw_latent_cache(key, part):
    keys = jax.random.split(jax.random.fold_in(key, 11), 1)
    values = jnp.clip(jax.random.normal(keys[0], (ROWS, CACHE, KL + R), jnp.float32), -6.0, 6.0)
    return values.astype(jnp.bfloat16)


def place_ends(entries, key, smallest, top_value):
    index_at = [jax.random.randint(jax.random.fold_in(key, axis), (), 0, length) for axis, length in enumerate(entries.shape)]
    longest = entries.shape.index(max(entries.shape))
    beside = index_at[:longest] + [(index_at[longest] + 1) % entries.shape[longest]] + index_at[longest + 1:]
    return entries.at[tuple(index_at)].set(smallest).at[tuple(beside)].set(top_value)


def spiked(values, rng, source, target, blocks, factor):
    def block_of(position):
        return (jnp.arange(values.shape[position]) // (values.shape[position] // blocks)).reshape((-1,) + (1,) * (values.ndim - 1 - position))

    first = jax.random.permutation(rng, blocks)[block_of(target)]
    other_side = (block_of(target) + blocks // 2) % blocks
    return jnp.where((block_of(source) == first) | (block_of(source) == other_side), factor * values, values)


def steps_of(stream_key, extent, cuts, smallest, largest):
    def one(axis_at, shards_of):
        heights = jax.random.uniform(jax.random.fold_in(jax.random.fold_in(stream_key, 6), axis_at), (shards_of,), jnp.float32, smallest / len(cuts), largest / len(cuts))
        return jnp.repeat(jnp.exp(heights), extent[axis_at] // shards_of).reshape((-1,) + (1,) * (len(extent) - axis_at - 1))

    level = one(*cuts[0])
    for cut in cuts[1:]:
        level = level * one(*cut)
    return level


def bell_draw(stream_key, extent, spread, reach, cuts=(), kind=jnp.bfloat16):
    array = jax.random.normal(stream_key, extent, jnp.float32) * spread
    if len(cuts) > 0:
        array = steps_of(stream_key, extent, cuts, -0.22, 0.18) * array
    return jnp.clip(array, min=-reach, max=reach).astype(kind)


def heavy_noise(key, extent, scale, most, cuts, heavy, kind=jnp.bfloat16):
    values = scale * jax.random.normal(key, extent, jnp.float32)
    if cuts:
        values = values * steps_of(key, extent, cuts, -0.22, 0.18)
    return jnp.clip(spiked(values, jax.random.fold_in(key, 3), *heavy), -most, most).astype(kind)


def setup_inputs(seed: int = 0) -> dict:
    seeds = jax.random.split(jax.random.key(seed), 16)
    return {
        "query_latent": bell_draw(seeds[0], (ROWS, STEPS, QR), 2.0, 12.0, ((0, 8),)),
        "new_entries": bell_draw(seeds[1], (ROWS, STEPS, KL + R), 1.0, 6.0, ((0, 8),)),
        "latent_cache": draw_latent_cache(jax.random.fold_in(seeds[15], 71), 0),
        "lengths": place_ends(jax.random.randint(seeds[3], (ROWS,), CACHE // 4, CACHE + 1), jax.random.fold_in(seeds[3], 1), CACHE // 4, CACHE).astype(jnp.int32),
        "query_up": bell_draw(seeds[4], (QR, H * HD), QR ** -0.5, 0.15625, ((0, 8), (1, 4)), jnp.float32),
        "key_up": bell_draw(seeds[5], (KL, H * HD), KL ** -0.5, 0.25, ((0, 8), (1, 4)), jnp.float32),
        "query_moment": bell_draw(seeds[6], (QR, H * HD), 0.5, 3.0, ((0, 8), (1, 4)), jnp.float32),
        "query_second": jnp.clip(jnp.exp(math.log(2.0) - 3.6888794 * jax.random.uniform(seeds[7], (QR, H * HD), jnp.float32) ** steps_of(seeds[7], (QR, H * HD), ((0, 8), (1, 4)), -0.2, 0.2)), 0.05, 2.0),
        "key_moment": bell_draw(seeds[8], (KL, H * HD), 0.5, 3.0, ((0, 8), (1, 4)), jnp.float32),
        "key_second": jnp.clip(jnp.exp(math.log(2.0) - 3.6888794 * jax.random.uniform(seeds[9], (KL, H * HD), jnp.float32) ** steps_of(seeds[9], (KL, H * HD), ((0, 8), (1, 4)), -0.2, 0.2)), 0.05, 2.0),
        "query_grads": bell_draw(seeds[10], (N_GROUP * N_INNER * QR, H * HD), 1.0, 6.0, ((0, 8), (1, 4))),
        "key_grads": bell_draw(seeds[11], (N_GROUP * N_INNER * KL, H * HD), 1.0, 6.0, ((0, 8), (1, 4))),
        "rope_query": bell_draw(seeds[12], (QR, H * R), QR ** -0.5, 0.15625, ((1, 4),)),
        "value_up": bell_draw(seeds[13], (KL, H * HD), KL ** -0.5, 0.25, ((1, 4),)),
        "output_weight": heavy_noise(seeds[14], (H * HD, D), (H * HD) ** -0.5, 0.25, ((0, 4),), (0, 1, 4, 2.0)),
    }


first_decay = 0.9
second_decay = 0.95
adam_epsilon = 1e-08
weight_decay = 0.1
learn_rate = 0.003
step_count = 10
rope_base = 10000.0

def optimizer_step(weight, moment, second, gradient):
    moment = first_decay * moment + (1.0 - first_decay) * gradient
    second = second_decay * second + (1.0 - second_decay) * gradient * gradient
    first_fix = 1.0 - first_decay ** step_count
    second_fix = 1.0 - second_decay ** step_count
    update = moment / first_fix / (jnp.sqrt(second / second_fix) + adam_epsilon)
    return (weight - learn_rate * (update + weight_decay * weight), moment, second)

def rotate(vectors, places):
    half_width = vectors.shape[-1] // 2
    frequency = rope_base ** (-jnp.arange(half_width, dtype=jnp.float32) / half_width)
    angles = places[..., None].astype(jnp.float32) * frequency
    cosine = jnp.cos(angles)
    sine_part = jnp.sin(angles)
    first_half = vectors[..., :half_width]
    second_half = vectors[..., half_width:]
    return jnp.concatenate([first_half * cosine - second_half * sine_part, first_half * sine_part + second_half * cosine], -1)

def reference(query_latent, new_entries, latent_cache, lengths, query_up, key_up, query_moment, query_second, key_moment, key_second, query_grads, key_grads, rope_query, value_up, output_weight):
    shard_count = query_grads.shape[0] // QR
    query_sum = lax.optimization_barrier(jnp.sum(query_grads.astype(jnp.float32).reshape(shard_count, QR, -1), 0))
    key_sum = lax.optimization_barrier(jnp.sum(key_grads.astype(jnp.float32).reshape(shard_count, KL, -1), 0))
    query_weight, query_first, query_square = optimizer_step(query_up, query_moment, query_second, query_sum)
    key_weight, key_first, key_square = optimizer_step(key_up, key_moment, key_second, key_sum)
    query_half = query_weight.astype(jnp.bfloat16)
    key_half = key_weight.astype(jnp.bfloat16)
    row_count = query_latent.shape[0]
    places = lengths[:, None] + jnp.arange(STEPS, dtype=jnp.int32)[None, :]
    new_rope = rotate(new_entries[:, :, KL:].astype(jnp.float32), places).astype(jnp.bfloat16)
    new_keys = jnp.concatenate([new_entries[:, :, :KL], new_rope], -1)
    flat_query = query_latent.reshape(row_count * STEPS, QR)
    live_mask = jnp.arange(CACHE, dtype=jnp.int32)[None, :] < lengths[:, None]
    causal = jnp.arange(STEPS, dtype=jnp.int32)[None, :] <= jnp.arange(STEPS, dtype=jnp.int32)[:, None]
    score_scale = 1.0 / math.sqrt(HD + R)
    cache_float = latent_cache.astype(jnp.float32)
    fresh_float = new_keys.astype(jnp.float32)

    def single_head(head_index):
        query_cols = lax.dynamic_slice_in_dim(query_half, head_index * HD, HD, 1)
        key_cols = lax.dynamic_slice_in_dim(key_half, head_index * HD, HD, 1)
        absorbed = jnp.dot(query_cols, key_cols.T, preferred_element_type=jnp.float32).astype(jnp.bfloat16)
        latent_query = jnp.dot(flat_query, absorbed, preferred_element_type=jnp.float32).astype(jnp.bfloat16)
        rope_cols = lax.dynamic_slice_in_dim(rope_query, head_index * R, R, 1)
        rope_part = jnp.dot(flat_query, rope_cols, preferred_element_type=jnp.float32).reshape(row_count, STEPS, R)
        rope_part = rotate(rope_part, places).astype(jnp.bfloat16)
        full_query = jnp.concatenate([latent_query.reshape(row_count, STEPS, KL), rope_part], -1).astype(jnp.float32)
        cache_scores = jnp.einsum('bsk,bck->bsc', full_query, cache_float) * score_scale
        fresh_scores = jnp.einsum('bsk,btk->bst', full_query, fresh_float) * score_scale
        cache_scores = jnp.where(live_mask[:, None, :], cache_scores, -jnp.inf)
        fresh_scores = jnp.where(causal[None], fresh_scores, -jnp.inf)
        highest = jnp.maximum(lax.optimization_barrier(jnp.max(cache_scores, -1)), lax.optimization_barrier(jnp.max(fresh_scores, -1)))
        cache_exp = jnp.exp(cache_scores - highest[..., None])
        fresh_exp = jnp.exp(fresh_scores - highest[..., None])
        denominator = lax.optimization_barrier(jnp.sum(cache_exp, -1)) + lax.optimization_barrier(jnp.sum(fresh_exp, -1))
        cache_probs = lax.optimization_barrier((cache_exp / denominator[..., None]).astype(jnp.bfloat16)).astype(jnp.float32)
        fresh_probs = lax.optimization_barrier((fresh_exp / denominator[..., None]).astype(jnp.bfloat16)).astype(jnp.float32)
        latent_out = jnp.einsum('bsc,bck->bsk', cache_probs, cache_float[:, :, :KL]) + jnp.einsum('bst,btk->bsk', fresh_probs, fresh_float[:, :, :KL])
        latent_out = latent_out.astype(jnp.bfloat16)
        value_cols = lax.dynamic_slice_in_dim(value_up, head_index * HD, HD, 1)
        return jnp.dot(latent_out.reshape(row_count * STEPS, KL), value_cols, preferred_element_type=jnp.float32).astype(jnp.bfloat16)
    head_outputs = lax.map(single_head, jnp.arange(H, dtype=jnp.int32))
    joined = jnp.transpose(head_outputs, (1, 0, 2)).reshape(row_count * STEPS, H * HD)
    attended = lax.dot_general(output_weight, joined, (((0,), (1,)), ((), ())), preferred_element_type=jnp.float32).astype(jnp.bfloat16)
    return (query_weight, key_weight, query_first, query_square, key_first, key_square, attended)
```

```python
import math

import jax
import jax.numpy as jnp
from jax import lax
from jax.sharding import PartitionSpec as P

QR = 1536
KL = 512
HD = 128
R = 64
HEAD_DEV = 2
STEPS = 3
CACHE = 512


first_decay = 0.9
second_decay = 0.95
adam_epsilon = 1e-08
weight_decay = 0.1
learn_rate = 0.003
step_count = 10
rope_base = 10000.0


def optimizer_step(weight, moment, second, gradient):
    moment = first_decay * moment + (1.0 - first_decay) * gradient
    second = second_decay * second + (1.0 - second_decay) * gradient * gradient
    first_fix = 1.0 - first_decay**step_count
    second_fix = 1.0 - second_decay**step_count
    update = moment / first_fix / (jnp.sqrt(second / second_fix) + adam_epsilon)
    return (weight - learn_rate * (update + weight_decay * weight), moment, second)


def rotate(vectors, places):
    half_width = vectors.shape[-1] // 2
    frequency = rope_base ** (-jnp.arange(half_width, dtype=jnp.float32) / half_width)
    angles = places[..., None].astype(jnp.float32) * frequency
    cosine = jnp.cos(angles)
    sine_part = jnp.sin(angles)
    first_half = vectors[..., :half_width]
    second_half = vectors[..., half_width:]
    return jnp.concatenate(
        [
            first_half * cosine - second_half * sine_part,
            first_half * sine_part + second_half * cosine,
        ],
        -1,
    )


ROW_AXES = ("group", "inner")


def swap(value, axes, count, distance):
    return lax.ppermute(value, axes, [(i, i ^ distance) for i in range(count)])


def block(value, index, axis=0):
    return lax.dynamic_index_in_dim(value, index, axis, keepdims=False)


def per_device(
    query_latent,
    new_entries,
    latent_cache,
    lengths,
    query_up,
    key_up,
    query_moment,
    query_second,
    key_moment,
    key_second,
    query_grads,
    key_grads,
    rope_query,
    value_up,
    output_weight,
):
    devices = lax.axis_size(ROW_AXES)
    chips = devices // 2
    me = lax.axis_index(ROW_AXES)
    chip, core = me // 2, me % 2
    row_count = query_latent.shape[0]
    flat_query = query_latent.reshape(row_count * STEPS, QR)
    tokens = row_count * STEPS
    query_rows, width = query_up.shape
    key_rows = key_up.shape[0]

    query_blocks = query_grads.reshape(chips, 2, query_rows, width)
    key_blocks = key_grads.reshape(chips, 2, key_rows, width)
    latent_blocks = flat_query.reshape(tokens, chips, 2, query_rows).transpose(1, 2, 0, 3)
    latent_blocks = jnp.pad(latent_blocks, ((0, 0), (0, 0), (0, 0), (0, width - query_rows)))
    give = jnp.concatenate(
        [block(x, 1 - core, 1) for x in (query_blocks, key_blocks, latent_blocks)], 1
    )
    got = swap(give, ROW_AXES, devices, 1)
    grad_rows = query_rows + key_rows
    chip_sum = jnp.concatenate(
        [block(query_blocks, core, 1), block(key_blocks, core, 1)], 1
    ).astype(jnp.float32) + got[:, :grad_rows].astype(jnp.float32)
    chip_pack = jnp.concatenate(
        [chip_sum.astype(jnp.bfloat16), block(latent_blocks, core, 1), got[:, grad_rows:]], 1
    )
    packs = [
        swap(block(chip_pack, chip ^ j), ROW_AXES, devices, 2 * j) for j in range(1, chips)
    ]
    total = block(chip_sum, chip)
    for pack in packs:
        total = total + pack[:grad_rows].astype(jnp.float32)
    latent_cols = jnp.stack(
        [x[grad_rows:, :query_rows] for x in [block(chip_pack, chip)] + packs]
    )
    query_weight, query_first, query_square = optimizer_step(
        query_up, query_moment, query_second, total[:query_rows]
    )
    key_weight, key_first, key_square = optimizer_step(
        key_up, key_moment, key_second, total[query_rows:]
    )
    query_half = query_weight.astype(jnp.bfloat16)
    key_half = key_weight.astype(jnp.bfloat16)

    partial = jnp.einsum(
        "jtr,rw->jtw", latent_cols, query_half, preferred_element_type=jnp.float32
    ).reshape(chips, 2, tokens, width)
    got_partial = swap(partial[:, 1].astype(jnp.bfloat16), ROW_AXES, devices, 1)
    got_key = swap(key_half, ROW_AXES, devices, 1)
    chip_partial = partial[:, 0] + got_partial.astype(jnp.float32)
    chip_keys = jnp.concatenate([key_half, got_key])
    half_partial = chip_partial.astype(jnp.bfloat16)
    packs = [
        swap(jnp.concatenate([half_partial[j], chip_keys]), ROW_AXES, devices, 2 * j)
        for j in range(1, chips)
    ]
    head_query = chip_partial[0]
    for pack in packs:
        head_query = head_query + pack[:tokens].astype(jnp.float32)
    head_query = head_query.astype(jnp.bfloat16)
    key_full = jnp.stack([chip_keys] + [pack[tokens:] for pack in packs])
    key_full = key_full.reshape(devices, key_rows, width)
    stage = 1
    while stage < devices:
        paired = key_full.reshape(devices // (2 * stage), 2, stage, key_rows, width)
        key_full = jnp.where((me & stage) != 0, paired[:, ::-1], paired)
        key_full = key_full.reshape(devices, key_rows, width)
        stage *= 2
    latent_query = jnp.einsum(
        "rhd,khd->rhk",
        head_query.reshape(tokens, HEAD_DEV, HD),
        key_full.reshape(KL, HEAD_DEV, HD),
        preferred_element_type=jnp.float32,
    )
    latent_query = latent_query.astype(jnp.bfloat16).reshape(row_count, STEPS, HEAD_DEV, KL)
    places = lengths[:, None] + jnp.arange(STEPS, dtype=jnp.int32)[None, :]
    rope_part = jnp.dot(flat_query, rope_query, preferred_element_type=jnp.float32).reshape(
        row_count, STEPS, HEAD_DEV, R
    )
    rope_part = rotate(rope_part, places[:, :, None]).astype(jnp.bfloat16)
    full_query = jnp.concatenate([latent_query, rope_part], -1)
    new_rope = rotate(new_entries[:, :, KL:].astype(jnp.float32), places).astype(jnp.bfloat16)
    new_keys = jnp.concatenate([new_entries[:, :, :KL], new_rope], -1)
    score_scale = 1.0 / math.sqrt(HD + R)
    cache_scores = (
        jnp.einsum("bshk,bck->bshc", full_query, latent_cache, preferred_element_type=jnp.float32)
        * score_scale
    )
    fresh_scores = (
        jnp.einsum("bshk,btk->bsht", full_query, new_keys, preferred_element_type=jnp.float32)
        * score_scale
    )
    live_mask = jnp.arange(CACHE, dtype=jnp.int32)[None, :] < lengths[:, None]
    causal = (
        jnp.arange(STEPS, dtype=jnp.int32)[None, :] <= jnp.arange(STEPS, dtype=jnp.int32)[:, None]
    )
    cache_scores = jnp.where(live_mask[:, None, None, :], cache_scores, -jnp.inf)
    fresh_scores = jnp.where(causal[None, :, None, :], fresh_scores, -jnp.inf)
    highest = jnp.maximum(jnp.max(cache_scores, -1), jnp.max(fresh_scores, -1))
    cache_exp = jnp.exp(cache_scores - highest[..., None])
    fresh_exp = jnp.exp(fresh_scores - highest[..., None])
    denominator = jnp.sum(cache_exp, -1) + jnp.sum(fresh_exp, -1)
    cache_probs = (cache_exp / denominator[..., None]).astype(jnp.bfloat16)
    fresh_probs = (fresh_exp / denominator[..., None]).astype(jnp.bfloat16)
    latent_out = jnp.einsum(
        "bshc,bck->bshk", cache_probs, latent_cache[:, :, :KL], preferred_element_type=jnp.float32
    )
    latent_out = latent_out + jnp.einsum(
        "bsht,btk->bshk", fresh_probs, new_keys[:, :, :KL], preferred_element_type=jnp.float32
    )
    latent_out = latent_out.astype(jnp.bfloat16)
    head_values = jnp.einsum(
        "bshk,khd->bshd",
        latent_out,
        value_up.reshape(KL, HEAD_DEV, HD),
        preferred_element_type=jnp.float32,
    )
    head_values = head_values.astype(jnp.bfloat16).reshape(row_count * STEPS, HEAD_DEV * HD)
    shares = lax.axis_size("fsdp")
    share = lax.axis_index("fsdp")
    partial_out = jnp.dot(head_values, output_weight, preferred_element_type=jnp.float32)
    partial_out = partial_out.reshape(tokens, shares, -1)
    half_out = partial_out.astype(jnp.bfloat16)
    packs = [
        swap(block(half_out, share ^ j, 1), "fsdp", shares, j) for j in range(1, shares)
    ]
    attended = block(partial_out, share, 1)
    for pack in packs:
        attended = attended + pack.astype(jnp.float32)
    attended = attended.astype(jnp.bfloat16).T
    return (query_weight, key_weight, query_first, query_square, key_first, key_square, attended)


def solution(mesh):
    return jax.shard_map(
        per_device,
        mesh=mesh,
        in_specs=(
            P(("group", "inner"), None, None),
            P(("group", "inner"), None, None),
            P(("group", "inner"), None, None),
            P(("group", "inner")),
            P(("group", "inner"), "fsdp"),
            P(("group", "inner"), "fsdp"),
            P(("group", "inner"), "fsdp"),
            P(("group", "inner"), "fsdp"),
            P(("group", "inner"), "fsdp"),
            P(("group", "inner"), "fsdp"),
            P(("group", "inner"), "fsdp"),
            P(("group", "inner"), "fsdp"),
            P(None, "fsdp"),
            P(None, "fsdp"),
            P("fsdp", None),
        ),
        out_specs=(
            P(("group", "inner"), "fsdp"),
            P(("group", "inner"), "fsdp"),
            P(("group", "inner"), "fsdp"),
            P(("group", "inner"), "fsdp"),
            P(("group", "inner"), "fsdp"),
            P(("group", "inner"), "fsdp"),
            P("fsdp", ("group", "inner")),
        ),
        check_vma=False,
    )
```

```python
import functools
import math

import jax
import jax.numpy as jnp
from jax import lax
from jax.experimental import pallas as pl
from jax.experimental.pallas import tpu as pltpu
from jax.sharding import PartitionSpec as P

QR = 1536
KL = 512
HD = 128
R = 64
STEPS = 3
CACHE = 512


first_decay = 0.9
second_decay = 0.95
adam_epsilon = 1e-08
weight_decay = 0.1
learn_rate = 0.003
step_count = 10
rope_base = 10000.0


def optimizer_step(weight, moment, second, gradient):
    moment = first_decay * moment + (1.0 - first_decay) * gradient
    second = second_decay * second + (1.0 - second_decay) * gradient * gradient
    first_fix = 1.0 - first_decay**step_count
    second_fix = 1.0 - second_decay**step_count
    update = moment / first_fix / (jnp.sqrt(second / second_fix) + adam_epsilon)
    return (weight - learn_rate * (update + weight_decay * weight), moment, second)


def rotate(vectors, places):
    half_width = vectors.shape[-1] // 2
    frequency = rope_base ** (-jnp.arange(half_width, dtype=jnp.float32) / half_width)
    angles = places[..., None].astype(jnp.float32) * frequency
    cosine = jnp.cos(angles)
    sine_part = jnp.sin(angles)
    first_half = vectors[..., :half_width]
    second_half = vectors[..., half_width:]
    return jnp.concatenate(
        [
            first_half * cosine - second_half * sine_part,
            first_half * sine_part + second_half * cosine,
        ],
        -1,
    )


ROW_AXES = ("group", "inner")


def swap(value, axes, count, distance):
    return lax.ppermute(value, axes, [(i, i ^ distance) for i in range(count)])


def block(value, index, axis=0):
    return lax.dynamic_index_in_dim(value, index, axis, keepdims=False)


def attend_kernel(
    rows, shares, whole_out,
    head_query, key_full, query_rope, new_keys, live, order, value_up, cache, weight, *outs,
):
    f32, bf16 = jnp.float32, jnp.bfloat16
    tokens = head_query.shape[0]
    heads = head_query.shape[1] // HD
    count = heads * tokens
    nt = (((1,), (1,)), ((), ()))
    nn = (((1,), (0,)), ((), ()))

    def dot(a, b, dims):
        return lax.dot_general(a, b, dims, preferred_element_type=f32)

    latent_query = jnp.concatenate(
        [
            dot(head_query[:, h * HD:(h + 1) * HD], key_full[:, h * HD:(h + 1) * HD], nt)
            for h in range(heads)
        ]
    ).astype(bf16)
    rope = query_rope[...]
    scale = 1.0 / math.sqrt(HD + R)
    row_of = lax.broadcasted_iota(jnp.int32, (count, 1), 0)
    batch_of, step_of = row_of % rows, (row_of // rows) % STEPS
    scores = jnp.zeros((count, CACHE), f32)
    for b in range(rows):
        here = dot(latent_query, cache[b, :KL, :], nn) + dot(rope, cache[b, KL:, :], nn)
        scores = jnp.where(batch_of == b, here, scores)
    slot = lax.broadcasted_iota(jnp.int32, (count, CACHE), 1)
    scores = jnp.where(slot < live[...], scores * scale, -jnp.inf)
    fresh = dot(latent_query, new_keys[:, :KL], nt) + dot(rope, new_keys[:, KL:], nt)
    key_at = lax.broadcasted_iota(jnp.int32, (count, tokens), 1)
    seen = (key_at % rows == batch_of) & (key_at // rows <= step_of)
    fresh = jnp.where(seen, fresh * scale, -jnp.inf)
    highest = jnp.maximum(
        jnp.max(scores, -1, keepdims=True), jnp.max(fresh, -1, keepdims=True)
    )
    scores, fresh = jnp.exp(scores - highest), jnp.exp(fresh - highest)
    denominator = jnp.sum(scores, -1, keepdims=True) + jnp.sum(fresh, -1, keepdims=True)
    probs = (scores / denominator).astype(bf16)
    latent_out = dot((fresh / denominator).astype(bf16), new_keys[:, :KL], nn)
    for b in range(rows):
        mine = jnp.where(batch_of == b, probs, jnp.zeros_like(probs))
        latent_out = latent_out + dot(mine, cache[b, :KL, :], nt)
    latent_out = latent_out.astype(bf16)
    head_values = jnp.concatenate(
        [
            dot(latent_out[h * tokens:(h + 1) * tokens], value_up[:, h * HD:(h + 1) * HD], nn)
            for h in range(heads)
        ],
        1,
    ).astype(bf16)
    head_values = dot(order[...], head_values, nn).astype(bf16)
    if whole_out:
        outs[0][...] = dot(head_values, weight[...], nn)
        return
    share = lax.axis_index("fsdp")
    part = weight.shape[1] // shares
    for j in range(shares):
        columns = pl.ds(pl.multiple_of((share ^ j) * part, 128), part)
        outs[j][...] = dot(head_values, weight[:, columns], nn).astype(outs[j].dtype)


def attend(head_query, key_full, query_rope, new_keys, lengths, value_up, cache, weight):
    rows = lengths.shape[0]
    tokens, columns = head_query.shape[0], weight.shape[1]
    heads = head_query.shape[1] // HD
    live = jnp.tile(lengths, heads * STEPS)[:, None]
    index = jnp.arange(tokens)
    order = ((index % STEPS) * rows + index // STEPS)[:, None] == index[None, :]
    shares = lax.axis_size("fsdp")
    part = columns // shares
    whole_out = part % 128 != 0
    if whole_out:
        outs = [jax.ShapeDtypeStruct((tokens, columns), jnp.float32)]
    else:
        outs = [
            jax.ShapeDtypeStruct((tokens, part), jnp.bfloat16 if j else jnp.float32)
            for j in range(shares)
        ]
    outs = pl.pallas_call(
        functools.partial(attend_kernel, rows, shares, whole_out),
        out_shape=outs,
        in_specs=[pl.BlockSpec(memory_space=pltpu.VMEM)] * 9,
        out_specs=[pl.BlockSpec(memory_space=pltpu.VMEM)] * len(outs),
        compiler_params=pltpu.CompilerParams(vmem_limit_bytes=24 << 20),
        name="attend",
    )(
        head_query, key_full, query_rope, new_keys, live, order.astype(jnp.bfloat16),
        value_up, cache, weight,
    )
    if whole_out:
        share = lax.axis_index("fsdp")
        blocks = outs[0].reshape(tokens, shares, part)
        own = block(blocks, share, 1)
        blocks = blocks.astype(jnp.bfloat16)
        return [own] + [block(blocks, share ^ j, 1) for j in range(1, shares)]
    return outs


def per_device(
    query_latent,
    new_entries,
    latent_cache,
    lengths,
    query_up,
    key_up,
    query_moment,
    query_second,
    key_moment,
    key_second,
    query_grads,
    key_grads,
    rope_query,
    value_up,
    output_weight,
):
    devices = lax.axis_size(ROW_AXES)
    chips = devices // 2
    me = lax.axis_index(ROW_AXES)
    chip, core = me // 2, me % 2
    row_count = query_latent.shape[0]
    flat_query = query_latent.transpose(1, 0, 2).reshape(row_count * STEPS, QR)
    tokens = row_count * STEPS
    query_rows, width = query_up.shape
    key_rows = key_up.shape[0]

    query_blocks = query_grads.reshape(chips, 2, query_rows, width)
    key_blocks = key_grads.reshape(chips, 2, key_rows, width)
    latent_blocks = flat_query.reshape(tokens, chips, 2, query_rows).transpose(1, 2, 0, 3)
    latent_blocks = jnp.pad(latent_blocks, ((0, 0), (0, 0), (0, 0), (0, width - query_rows)))
    give = jnp.concatenate(
        [block(x, 1 - core, 1) for x in (query_blocks, key_blocks, latent_blocks)], 1
    )
    got = swap(give, ROW_AXES, devices, 1)
    grad_rows = query_rows + key_rows
    chip_sum = jnp.concatenate(
        [block(query_blocks, core, 1), block(key_blocks, core, 1)], 1
    ).astype(jnp.float32) + got[:, :grad_rows].astype(jnp.float32)
    chip_pack = jnp.concatenate(
        [chip_sum.astype(jnp.bfloat16), block(latent_blocks, core, 1), got[:, grad_rows:]], 1
    )
    packs = [
        swap(block(chip_pack, chip ^ j), ROW_AXES, devices, 2 * j) for j in range(1, chips)
    ]
    total = block(chip_sum, chip)
    for pack in packs:
        total = total + pack[:grad_rows].astype(jnp.float32)
    latent_cols = jnp.stack(
        [x[grad_rows:, :query_rows] for x in [block(chip_pack, chip)] + packs]
    )
    query_weight, query_first, query_square = optimizer_step(
        query_up, query_moment, query_second, total[:query_rows]
    )
    key_weight, key_first, key_square = optimizer_step(
        key_up, key_moment, key_second, total[query_rows:]
    )
    query_half = query_weight.astype(jnp.bfloat16)
    key_half = key_weight.astype(jnp.bfloat16)

    partial = jnp.einsum(
        "jtr,rw->jtw", latent_cols, query_half, preferred_element_type=jnp.float32
    ).reshape(chips, 2, tokens, width)
    got_partial = swap(partial[:, 1].astype(jnp.bfloat16), ROW_AXES, devices, 1)
    got_key = swap(key_half, ROW_AXES, devices, 1)
    chip_partial = partial[:, 0] + got_partial.astype(jnp.float32)
    chip_keys = jnp.concatenate([key_half, got_key])
    half_partial = chip_partial.astype(jnp.bfloat16)
    packs = [
        swap(jnp.concatenate([half_partial[j], chip_keys]), ROW_AXES, devices, 2 * j)
        for j in range(1, chips)
    ]
    head_query = chip_partial[0]
    for pack in packs:
        head_query = head_query + pack[:tokens].astype(jnp.float32)
    head_query = head_query.astype(jnp.bfloat16)
    key_full = jnp.stack([chip_keys] + [pack[tokens:] for pack in packs])
    key_full = key_full.reshape(devices, key_rows, width)
    stage = 1
    while stage < devices:
        paired = key_full.reshape(devices // (2 * stage), 2, stage, key_rows, width)
        key_full = jnp.where((me & stage) != 0, paired[:, ::-1], paired)
        key_full = key_full.reshape(devices, key_rows, width)
        stage *= 2
    key_full = key_full.reshape(KL, width)
    places = (lengths[None, :] + jnp.arange(STEPS, dtype=jnp.int32)[:, None]).reshape(tokens)
    query_rope = jnp.dot(flat_query, rope_query, preferred_element_type=jnp.float32)
    query_rope = query_rope.reshape(tokens, -1, R).transpose(1, 0, 2)
    query_rope = rotate(query_rope, places[None]).astype(jnp.bfloat16).reshape(-1, R)
    entries = new_entries.transpose(1, 0, 2).reshape(tokens, KL + R)
    new_rope = rotate(entries[:, KL:].astype(jnp.float32), places).astype(jnp.bfloat16)
    new_keys = jnp.concatenate([entries[:, :KL], new_rope], -1)
    cache, weight = latent_cache.transpose(0, 2, 1), output_weight
    attended, *give = attend(
        head_query, key_full, query_rope, new_keys, lengths, value_up, cache, weight
    )
    shares = lax.axis_size("fsdp")
    packs = [swap(pack, "fsdp", shares, j + 1) for j, pack in enumerate(give)]
    for pack in packs:
        attended = attended + pack.astype(jnp.float32)
    attended = attended.astype(jnp.bfloat16).T
    return (query_weight, key_weight, query_first, query_square, key_first, key_square, attended)


def solution(mesh):
    return jax.shard_map(
        per_device,
        mesh=mesh,
        in_specs=(
            P(("group", "inner"), None, None),
            P(("group", "inner"), None, None),
            P(("group", "inner"), None, None),
            P(("group", "inner")),
            P(("group", "inner"), "fsdp"),
            P(("group", "inner"), "fsdp"),
            P(("group", "inner"), "fsdp"),
            P(("group", "inner"), "fsdp"),
            P(("group", "inner"), "fsdp"),
            P(("group", "inner"), "fsdp"),
            P(("group", "inner"), "fsdp"),
            P(("group", "inner"), "fsdp"),
            P(None, "fsdp"),
            P(None, "fsdp"),
            P("fsdp", None),
        ),
        out_specs=(
            P(("group", "inner"), "fsdp"),
            P(("group", "inner"), "fsdp"),
            P(("group", "inner"), "fsdp"),
            P(("group", "inner"), "fsdp"),
            P(("group", "inner"), "fsdp"),
            P(("group", "inner"), "fsdp"),
            P("fsdp", ("group", "inner")),
        ),
        check_vma=False,
    )
```

```python
import functools
import math

import jax
import jax.numpy as jnp
from jax import lax
from jax.experimental import pallas as pl
from jax.experimental.pallas import tpu as pltpu
from jax.sharding import PartitionSpec as P

QR = 1536
KL = 512
HD = 128
R = 64
STEPS = 3
CACHE = 512


first_decay = 0.9
second_decay = 0.95
adam_epsilon = 1e-08
weight_decay = 0.1
learn_rate = 0.003
step_count = 10
rope_base = 10000.0


def optimizer_step(weight, moment, second, gradient):
    moment = first_decay * moment + (1.0 - first_decay) * gradient
    second = second_decay * second + (1.0 - second_decay) * gradient * gradient
    first_fix = 1.0 - first_decay**step_count
    second_fix = 1.0 - second_decay**step_count
    update = moment / first_fix / (jnp.sqrt(second / second_fix) + adam_epsilon)
    return (weight - learn_rate * (update + weight_decay * weight), moment, second)


def rotate(vectors, places):
    half_width = vectors.shape[-1] // 2
    frequency = rope_base ** (-jnp.arange(half_width, dtype=jnp.float32) / half_width)
    angles = places[..., None].astype(jnp.float32) * frequency
    cosine = jnp.cos(angles)
    sine_part = jnp.sin(angles)
    first_half = vectors[..., :half_width]
    second_half = vectors[..., half_width:]
    return jnp.concatenate(
        [
            first_half * cosine - second_half * sine_part,
            first_half * sine_part + second_half * cosine,
        ],
        -1,
    )


ROW_AXES = ("group", "inner")


def swap(value, axes, count, distance):
    return lax.ppermute(value, axes, [(i, i ^ distance) for i in range(count)])


def block(value, index, axis=0):
    return lax.dynamic_index_in_dim(value, index, axis, keepdims=False)


VMEM_SPEC = pl.BlockSpec(memory_space=pltpu.VMEM)
HBM_SPEC = pl.BlockSpec(memory_space=pltpu.HBM)


def in_hbm(value):
    return pltpu.with_memory_space_constraint(value, pltpu.HBM)


def place():
    me = lax.axis_index(ROW_AXES)
    return me // 2, me % 2, lax.axis_size(ROW_AXES) // 2


def rows_at(index, count):
    return pl.ds(pl.multiple_of(index * count, 16), count)


def own_kernel(query_own, key_own, out, sems):
    chip, core, chips = place()
    copies = []
    for other in range(chips):
        start = 0
        for i, own in enumerate((query_own, key_own)):
            count = own.shape[0] // (2 * chips)
            copies.append(
                pltpu.make_async_copy(
                    own.at[rows_at(2 * other + core, count), :],
                    out.at[other, pl.ds(start, count), :],
                    sems.at[2 * other + i],
                )
            )
            start += count
    for copy in copies:
        copy.start()
    for copy in copies:
        copy.wait()


def own_blocks(query_own, key_own):
    chips = lax.axis_size(ROW_AXES) // 2
    grad_rows = (query_own.shape[0] + key_own.shape[0]) // (2 * chips)
    return pl.pallas_call(
        own_kernel,
        out_shape=jax.ShapeDtypeStruct((chips, grad_rows, query_own.shape[1]), query_own.dtype),
        in_specs=[HBM_SPEC] * 2,
        out_specs=VMEM_SPEC,
        scratch_shapes=[pltpu.SemaphoreType.DMA((2 * chips,))],
        compiler_params=pltpu.CompilerParams(vmem_limit_bytes=2 << 20),
        cost_estimate=pl.CostEstimate(flops=10**9, bytes_accessed=10**6, transcendentals=0),
        name="own",
    )(in_hbm(query_own), in_hbm(key_own))


def pack_kernel(own, query_got, key_got, latent_own, latent_got, *outs):
    chip, core, chips = place()
    total, latent_out, packs = outs[0], outs[1], outs[2:]
    grad_rows = total.shape[0]
    for j in range(chips):
        other = chip ^ j
        start = 0
        for got in (query_got, key_got):
            count = got.shape[0] // (2 * chips)
            both = own[other, start:start + count, :].astype(jnp.float32)
            both = both + got[rows_at(2 * other + core, count), :].astype(jnp.float32)
            if j == 0:
                total[start:start + count, :] = both
            else:
                packs[j - 1][start:start + count, :] = both.astype(jnp.bfloat16)
            start += count
        latents = jnp.concatenate(
            [latent_own[other].astype(jnp.float32), latent_got[other].astype(jnp.float32)]
        ).astype(jnp.bfloat16)
        if j == 0:
            latent_out[...] = latents
        else:
            packs[j - 1][grad_rows:, :] = latents


def pack_sums(own, query_got, key_got, latent_own, latent_got):
    chips, grad_rows, width = own.shape
    tokens = latent_own.shape[1]
    total, latents, *packs = pl.pallas_call(
        pack_kernel,
        out_shape=[
            jax.ShapeDtypeStruct((grad_rows, width), jnp.float32),
            jax.ShapeDtypeStruct((2 * tokens, width), jnp.bfloat16),
        ]
        + [jax.ShapeDtypeStruct((grad_rows + 2 * tokens, width), jnp.bfloat16)] * (chips - 1),
        in_specs=[VMEM_SPEC] * 5,
        out_specs=[VMEM_SPEC] * (chips + 1),
        compiler_params=pltpu.CompilerParams(vmem_limit_bytes=8 << 20),
        cost_estimate=pl.CostEstimate(flops=10**9, bytes_accessed=10**6, transcendentals=0),
        name="pack",
    )(own, query_got, key_got, latent_own, latent_got)
    return total, latents, packs


def update_kernel(chips, *refs):
    total, latents = refs[:2]
    packs, refs = refs[2:chips + 1], refs[chips + 1:]
    states, outs = refs[:6], refs[6:]
    partial, gives = outs[6], outs[7:]
    grad_rows = total.shape[0]
    gradient = total[...]
    for got in packs:
        gradient = gradient + got[:grad_rows, :].astype(jnp.float32)
    start = 0
    halves = []
    for i in range(2):
        weight, moment, second = states[3 * i:3 * i + 3]
        count = weight.shape[0]
        new = optimizer_step(
            weight[...], moment[...], second[...], gradient[start:start + count]
        )
        for out, value in zip(outs[3 * i:3 * i + 3], new):
            out[...] = value
        halves.append(new[0].astype(jnp.bfloat16))
        start += count
    query_half, key_half = halves
    query_rows = query_half.shape[0]
    tokens = partial.shape[0]
    for j in range(chips):
        columns = latents[:, :query_rows] if j == 0 else packs[j - 1][grad_rows:, :query_rows]
        product = jnp.dot(columns, query_half, preferred_element_type=jnp.float32)
        if j == 0:
            partial[...] = product
        else:
            gives[j][:tokens, :] = product.astype(jnp.bfloat16)
            gives[j][tokens:, :] = key_half
    gives[0][...] = key_half


def update(total, latents, packs, states):
    chips = len(packs) + 1
    tokens, width = latents.shape
    key_rows = states[3].shape[0]
    *outs, = pl.pallas_call(
        functools.partial(update_kernel, chips),
        out_shape=[jax.ShapeDtypeStruct(x.shape, x.dtype) for x in states]
        + [
            jax.ShapeDtypeStruct((tokens, width), jnp.float32),
            jax.ShapeDtypeStruct((key_rows, width), jnp.bfloat16),
        ]
        + [jax.ShapeDtypeStruct((tokens + key_rows, width), jnp.bfloat16)] * (chips - 1),
        in_specs=[VMEM_SPEC] * (chips + 7),
        out_specs=[VMEM_SPEC] * (chips + 7),
        compiler_params=pltpu.CompilerParams(vmem_limit_bytes=8 << 20),
        cost_estimate=pl.CostEstimate(flops=10**9, bytes_accessed=10**6, transcendentals=0),
        name="update",
    )(total, latents, *packs, *states)
    return outs[:6], outs[6], outs[7], outs[8:]


def merge_kernel(partial, key_half, *refs):
    *gots, query_sum, pair = refs
    tokens = partial.shape[0] // 2
    key_rows = key_half.shape[0]
    total = partial[...]
    pair[:key_rows, :] = key_half[...]
    for j, got in enumerate(gots):
        total = total + got[:2 * tokens, :].astype(jnp.float32)
        pair[(j + 1) * key_rows:(j + 2) * key_rows, :] = got[2 * tokens:, :]
    query_sum[...] = total[:tokens]
    pair[(len(gots) + 1) * key_rows:, :] = total[tokens:].astype(jnp.bfloat16)


def merge(partial, key_half, gots):
    tokens, width = partial.shape
    rows = (len(gots) + 1) * key_half.shape[0] + tokens // 2
    return pl.pallas_call(
        merge_kernel,
        out_shape=[
            jax.ShapeDtypeStruct((tokens // 2, width), jnp.float32),
            jax.ShapeDtypeStruct((rows, width), jnp.bfloat16),
        ],
        in_specs=[VMEM_SPEC] * (len(gots) + 2),
        out_specs=[VMEM_SPEC] * 2,
        compiler_params=pltpu.CompilerParams(vmem_limit_bytes=2 << 20),
        name="merge",
    )(partial, key_half, *gots)


def attend_kernel(
    rows, shares, whole_out,
    query_sum, pair_own, pair_got, query_rope, new_keys, live, order, value_up, cache_in, weight_in,
    *outs,
):
    f32, bf16 = jnp.float32, jnp.bfloat16
    *outs, key_full, cache, weight, sems = outs
    copies = [
        pltpu.make_async_copy(cache_in.at[b], cache.at[b], sems.at[b]) for b in range(rows)
    ]
    copies.append(pltpu.make_async_copy(weight_in, weight, sems.at[rows]))
    for copy in copies:
        copy.start()
    tokens = query_sum.shape[0]
    heads = query_sum.shape[1] // HD
    count = heads * tokens
    chip, core, chips = place()
    key_rows = KL // (2 * chips)
    for j in range(chips):
        for pair, side in ((pair_own, core), (pair_got, 1 - core)):
            at = rows_at(2 * (chip ^ j) + side, key_rows)
            key_full[at, :] = pair[j * key_rows:(j + 1) * key_rows, :]
    head_query = (query_sum[...] + pair_got[KL // 2:, :].astype(f32)).astype(bf16)
    nt = (((1,), (1,)), ((), ()))
    nn = (((1,), (0,)), ((), ()))

    def dot(a, b, dims):
        return lax.dot_general(a, b, dims, preferred_element_type=f32)

    latent_query = jnp.concatenate(
        [
            dot(head_query[:, h * HD:(h + 1) * HD], key_full[:, h * HD:(h + 1) * HD], nt)
            for h in range(heads)
        ]
    ).astype(bf16)
    rope = query_rope[...]
    scale = 1.0 / math.sqrt(HD + R)
    row_of = lax.broadcasted_iota(jnp.int32, (count, 1), 0)
    batch_of, step_of = row_of % rows, (row_of // rows) % STEPS
    scores = jnp.zeros((count, CACHE), f32)
    for b in range(rows):
        copies[b].wait()
        here = dot(latent_query, cache[b, :KL, :], nn) + dot(rope, cache[b, KL:, :], nn)
        scores = jnp.where(batch_of == b, here, scores)
    slot = lax.broadcasted_iota(jnp.int32, (count, CACHE), 1)
    scores = jnp.where(slot < live[...], scores * scale, -jnp.inf)
    fresh = dot(latent_query, new_keys[:, :KL], nt) + dot(rope, new_keys[:, KL:], nt)
    key_at = lax.broadcasted_iota(jnp.int32, (count, tokens), 1)
    seen = (key_at % rows == batch_of) & (key_at // rows <= step_of)
    fresh = jnp.where(seen, fresh * scale, -jnp.inf)
    highest = jnp.maximum(
        jnp.max(scores, -1, keepdims=True), jnp.max(fresh, -1, keepdims=True)
    )
    scores, fresh = jnp.exp(scores - highest), jnp.exp(fresh - highest)
    denominator = jnp.sum(scores, -1, keepdims=True) + jnp.sum(fresh, -1, keepdims=True)
    probs = (scores / denominator).astype(bf16)
    latent_out = dot((fresh / denominator).astype(bf16), new_keys[:, :KL], nn)
    for b in range(rows):
        mine = jnp.where(batch_of == b, probs, jnp.zeros_like(probs))
        latent_out = latent_out + dot(mine, cache[b, :KL, :], nt)
    latent_out = latent_out.astype(bf16)
    head_values = jnp.concatenate(
        [
            dot(latent_out[h * tokens:(h + 1) * tokens], value_up[:, h * HD:(h + 1) * HD], nn)
            for h in range(heads)
        ],
        1,
    ).astype(bf16)
    head_values = dot(order[...], head_values, nn).astype(bf16)
    copies[rows].wait()
    if whole_out:
        outs[0][...] = dot(head_values, weight[...], nn)
        return
    share = lax.axis_index("fsdp")
    part = weight.shape[1] // shares
    for j in range(shares):
        columns = pl.ds(pl.multiple_of((share ^ j) * part, 128), part)
        outs[j][...] = dot(head_values, weight[:, columns], nn).astype(outs[j].dtype)


def attend(
    query_sum, pair_own, pair_got, query_rope, new_keys, lengths, value_up, cache, weight
):
    rows = lengths.shape[0]
    tokens, columns = rows * STEPS, weight.shape[1]
    width = query_sum.shape[1]
    heads = width // HD
    live = jnp.tile(lengths, heads * STEPS)[:, None]
    index = jnp.arange(tokens)
    order = ((index % STEPS) * rows + index // STEPS)[:, None] == index[None, :]
    shares = lax.axis_size("fsdp")
    part = columns // shares
    whole_out = part % 128 != 0
    if whole_out:
        outs = [jax.ShapeDtypeStruct((tokens, columns), jnp.float32)]
    else:
        outs = [
            jax.ShapeDtypeStruct((tokens, part), jnp.bfloat16 if j else jnp.float32)
            for j in range(shares)
        ]
    outs = pl.pallas_call(
        functools.partial(attend_kernel, rows, shares, whole_out),
        out_shape=outs,
        in_specs=[VMEM_SPEC] * 8 + [HBM_SPEC] * 2,
        out_specs=[VMEM_SPEC] * len(outs),
        scratch_shapes=[
            pltpu.VMEM((KL, width), jnp.bfloat16),
            pltpu.VMEM(cache.shape, cache.dtype),
            pltpu.VMEM(weight.shape, weight.dtype),
            pltpu.SemaphoreType.DMA((rows + 1,)),
        ],
        compiler_params=pltpu.CompilerParams(vmem_limit_bytes=24 << 20),
        name="attend",
    )(
        query_sum, pair_own, pair_got, query_rope, new_keys, live, order.astype(jnp.bfloat16),
        value_up, in_hbm(cache), in_hbm(weight),
    )
    if whole_out:
        share = lax.axis_index("fsdp")
        blocks = outs[0].reshape(tokens, shares, part)
        own = block(blocks, share, 1)
        blocks = blocks.astype(jnp.bfloat16)
        return [own] + [block(blocks, share ^ j, 1) for j in range(1, shares)]
    return outs


def per_device(
    query_latent,
    new_entries,
    latent_cache,
    lengths,
    query_up,
    key_up,
    query_moment,
    query_second,
    key_moment,
    key_second,
    query_grads,
    key_grads,
    rope_query,
    value_up,
    output_weight,
):
    chip, core, chips = place()
    devices = 2 * chips
    row_count = query_latent.shape[0]
    tokens = row_count * STEPS
    flat_query = query_latent.transpose(1, 0, 2).reshape(tokens, QR)
    query_rows, width = query_up.shape
    key_rows = key_up.shape[0]

    query_got = swap(query_grads, ROW_AXES, devices, 1)
    key_got = swap(key_grads, ROW_AXES, devices, 1)
    latents = flat_query.reshape(tokens, chips, 2, query_rows).transpose(1, 2, 0, 3)
    latents = jnp.pad(latents, ((0, 0), (0, 0), (0, 0), (0, width - query_rows)))
    latent_got = swap(block(latents, 1 - core, 1), ROW_AXES, devices, 1)
    total, columns, packs = pack_sums(
        own_blocks(query_grads, key_grads), query_got, key_got, block(latents, core, 1), latent_got
    )
    packs = [swap(pack, ROW_AXES, devices, 2 * j + 2) for j, pack in enumerate(packs)]

    states = (query_up, query_moment, query_second, key_up, key_moment, key_second)
    states, query_sum, key_half, gives = update(total, columns, packs, states)
    query_weight, query_first, query_square, key_weight, key_first, key_square = states
    gots = [swap(give, ROW_AXES, devices, 2 * j + 2) for j, give in enumerate(gives)]
    query_sum, pair_own = merge(query_sum, key_half, gots)
    pair_got = swap(pair_own, ROW_AXES, devices, 1)
    places = (lengths[None, :] + jnp.arange(STEPS, dtype=jnp.int32)[:, None]).reshape(tokens)
    query_rope = jnp.dot(flat_query, rope_query, preferred_element_type=jnp.float32)
    query_rope = query_rope.reshape(tokens, -1, R).transpose(1, 0, 2)
    query_rope = rotate(query_rope, places[None]).astype(jnp.bfloat16).reshape(-1, R)
    entries = new_entries.transpose(1, 0, 2).reshape(tokens, KL + R)
    new_rope = rotate(entries[:, KL:].astype(jnp.float32), places).astype(jnp.bfloat16)
    new_keys = jnp.concatenate([entries[:, :KL], new_rope], -1)
    cache, weight = latent_cache.transpose(0, 2, 1), output_weight
    attended, *give = attend(
        query_sum, pair_own, pair_got, query_rope, new_keys, lengths, value_up, cache, weight
    )
    shares = lax.axis_size("fsdp")
    packs = [swap(pack, "fsdp", shares, j + 1) for j, pack in enumerate(give)]
    for pack in packs:
        attended = attended + pack.astype(jnp.float32)
    attended = attended.astype(jnp.bfloat16).T
    return (query_weight, key_weight, query_first, query_square, key_first, key_square, attended)


def solution(mesh):
    return jax.shard_map(
        per_device,
        mesh=mesh,
        in_specs=(
            P(("group", "inner"), None, None),
            P(("group", "inner"), None, None),
            P(("group", "inner"), None, None),
            P(("group", "inner")),
            P(("group", "inner"), "fsdp"),
            P(("group", "inner"), "fsdp"),
            P(("group", "inner"), "fsdp"),
            P(("group", "inner"), "fsdp"),
            P(("group", "inner"), "fsdp"),
            P(("group", "inner"), "fsdp"),
            P(("group", "inner"), "fsdp"),
            P(("group", "inner"), "fsdp"),
            P(None, "fsdp"),
            P(None, "fsdp"),
            P("fsdp", None),
        ),
        out_specs=(
            P(("group", "inner"), "fsdp"),
            P(("group", "inner"), "fsdp"),
            P(("group", "inner"), "fsdp"),
            P(("group", "inner"), "fsdp"),
            P(("group", "inner"), "fsdp"),
            P(("group", "inner"), "fsdp"),
            P("fsdp", ("group", "inner")),
        ),
        check_vma=False,
    )
```

```python
import functools
import math

import jax
import jax.numpy as jnp
from jax import lax
from jax.experimental import pallas as pl
from jax.experimental.pallas import tpu as pltpu
from jax.sharding import PartitionSpec as P


QR = 1536
KL = 512
HD = 128
R = 64
STEPS = 3
CACHE = 512


first_decay = 0.9
second_decay = 0.95
adam_epsilon = 1e-08
weight_decay = 0.1
learn_rate = 0.003
step_count = 10
rope_base = 10000.0


def optimizer_step(weight, moment, second, gradient):
    moment = first_decay * moment + (1.0 - first_decay) * gradient
    second = second_decay * second + (1.0 - second_decay) * gradient * gradient
    first_fix = 1.0 - first_decay**step_count
    second_fix = 1.0 - second_decay**step_count
    update = moment / first_fix / (jnp.sqrt(second / second_fix) + adam_epsilon)
    return (weight - learn_rate * (update + weight_decay * weight), moment, second)


ROW_AXES = ("group", "inner")


def swap(value, axes, count, distance):
    return lax.ppermute(value, axes, [(i, i ^ distance) for i in range(count)])


def block(value, index, axis=0):
    return lax.dynamic_index_in_dim(value, index, axis, keepdims=False)


VMEM_SPEC = pl.BlockSpec(memory_space=pltpu.VMEM)
HBM_SPEC = pl.BlockSpec(memory_space=pltpu.HBM)


def in_hbm(value):
    return pltpu.with_memory_space_constraint(value, pltpu.HBM)


def place():
    me = lax.axis_index(ROW_AXES)
    return me // 2, me % 2, lax.axis_size(ROW_AXES) // 2


def rows_at(index, count):
    return pl.ds(pl.multiple_of(index * count, 16), count)


def own_kernel(query_own, key_own, latents, out, keep, give, sems):
    _, core, chips = place()
    copies = []
    for other in range(chips):
        start = 0
        for i, own in enumerate((query_own, key_own)):
            count = own.shape[0] // (2 * chips)
            copies.append(
                pltpu.make_async_copy(
                    own.at[rows_at(2 * other + core, count), :],
                    out.at[other, pl.ds(start, count), :],
                    sems.at[2 * other + i],
                )
            )
            start += count
    for copy in copies:
        copy.start()
    count = query_own.shape[0] // (2 * chips)
    values = latents[...].astype(jnp.float32)
    pad = jnp.zeros((values.shape[0], keep.shape[2] - count), jnp.float32)
    for other in range(chips):
        even, odd = (
            jnp.concatenate(
                [values[:, (2 * other + i) * count:(2 * other + i + 1) * count], pad], 1
            )
            for i in range(2)
        )
        keep[other] = jnp.where(core == 0, even, odd).astype(keep.dtype)
        give[other] = jnp.where(core == 0, odd, even).astype(give.dtype)
    for copy in copies:
        copy.wait()


def own_blocks(query_own, key_own, latents):
    chips = lax.axis_size(ROW_AXES) // 2
    width = query_own.shape[1]
    grad_rows = (query_own.shape[0] + key_own.shape[0]) // (2 * chips)
    return pl.pallas_call(
        own_kernel,
        out_shape=[jax.ShapeDtypeStruct((chips, grad_rows, width), query_own.dtype)]
        + [jax.ShapeDtypeStruct((chips, latents.shape[0], width), latents.dtype)] * 2,
        in_specs=[HBM_SPEC] * 2 + [VMEM_SPEC],
        out_specs=[VMEM_SPEC] * 3,
        scratch_shapes=[pltpu.SemaphoreType.DMA((2 * chips,))],
        compiler_params=pltpu.CompilerParams(vmem_limit_bytes=2 << 20),
        cost_estimate=pl.CostEstimate(flops=10**9, bytes_accessed=10**6, transcendentals=0),
        name="own",
    )(in_hbm(query_own), in_hbm(key_own), latents)


def pack_kernel(own, query_got, key_got, latent_own, latent_got, *outs):
    chip, core, chips = place()
    total, latent_out, packs = outs[0], outs[1], outs[2:]
    grad_rows = total.shape[0]
    for j in range(chips):
        other = chip ^ j
        start = 0
        for got in (query_got, key_got):
            count = got.shape[0] // (2 * chips)
            both = own[other, start:start + count, :].astype(jnp.float32)
            both = both + got[rows_at(2 * other + core, count), :].astype(jnp.float32)
            if j == 0:
                total[start:start + count, :] = both
            else:
                packs[j - 1][start:start + count, :] = both.astype(jnp.bfloat16)
            start += count
        latents = jnp.concatenate(
            [latent_own[other].astype(jnp.float32), latent_got[other].astype(jnp.float32)]
        ).astype(jnp.bfloat16)
        if j == 0:
            latent_out[...] = latents
        else:
            packs[j - 1][grad_rows:, :] = latents


def pack_sums(own, query_got, key_got, latent_own, latent_got):
    chips, grad_rows, width = own.shape
    tokens = latent_own.shape[1]
    total, latents, *packs = pl.pallas_call(
        pack_kernel,
        out_shape=[
            jax.ShapeDtypeStruct((grad_rows, width), jnp.float32),
            jax.ShapeDtypeStruct((2 * tokens, width), jnp.bfloat16),
        ]
        + [jax.ShapeDtypeStruct((grad_rows + 2 * tokens, width), jnp.bfloat16)] * (chips - 1),
        in_specs=[VMEM_SPEC] * 5,
        out_specs=[VMEM_SPEC] * (chips + 1),
        compiler_params=pltpu.CompilerParams(vmem_limit_bytes=8 << 20),
        cost_estimate=pl.CostEstimate(flops=10**9, bytes_accessed=10**6, transcendentals=0),
        name="pack",
    )(own, query_got, key_got, latent_own, latent_got)
    return total, latents, packs


def row_value(lengths, count, rows):
    token = lax.broadcasted_iota(jnp.int32, (count, rows), 0)
    row = lax.broadcasted_iota(jnp.int32, (count, rows), 1)
    return jnp.sum(jnp.where(token % rows == row, lengths, 0), 1, keepdims=True)


def rope_kernel(after, query, weight, entries, lengths, query_rope, new_keys):
    del after
    tokens, rows = query.shape[0], lengths.shape[1]
    half = R // 2
    step = lax.broadcasted_iota(jnp.int32, (tokens, 1), 0) // rows
    place_of = (row_value(lengths[...], tokens, rows) + step).astype(jnp.float32)
    index = lax.broadcasted_iota(jnp.int32, (tokens, half), 1).astype(jnp.float32)
    angles = place_of * jnp.exp(index * (-math.log(rope_base) / half))
    cosine, sine = jnp.cos(angles), jnp.sin(angles)

    def turn(vectors):
        first, second = vectors[:, :half], vectors[:, half:]
        return jnp.concatenate(
            [first * cosine - second * sine, first * sine + second * cosine], 1
        )

    projected = jnp.dot(query[...], weight[...], preferred_element_type=jnp.float32)
    heads = projected.shape[1] // R
    query_rope[...] = jnp.concatenate(
        [turn(projected[:, h * R:(h + 1) * R]) for h in range(heads)]
    ).astype(jnp.bfloat16)
    new_keys[:, :KL] = entries[:, :KL]
    new_keys[:, KL:] = turn(entries[:, KL:].astype(jnp.float32)).astype(jnp.bfloat16)


def rope(after, query, weight, entries, lengths):
    heads = weight.shape[1] // R
    return pl.pallas_call(
        rope_kernel,
        out_shape=[
            jax.ShapeDtypeStruct((heads * query.shape[0], R), jnp.bfloat16),
            jax.ShapeDtypeStruct(entries.shape, jnp.bfloat16),
        ],
        in_specs=[VMEM_SPEC] * 5,
        out_specs=[VMEM_SPEC] * 2,
        compiler_params=pltpu.CompilerParams(vmem_limit_bytes=4 << 20),
        name="rope",
    )(after, query, weight, entries, lengths)


def update_kernel(chips, *refs):
    total, latents = refs[:2]
    packs, refs = refs[2:chips + 1], refs[chips + 1:]
    states, outs = refs[:6], refs[6:]
    partial, gives = outs[6], outs[7:]
    grad_rows = total.shape[0]
    gradient = total[...]
    for got in packs:
        gradient = gradient + got[:grad_rows, :].astype(jnp.float32)
    start = 0
    halves = []
    for i in range(2):
        weight, moment, second = states[3 * i:3 * i + 3]
        count = weight.shape[0]
        new = optimizer_step(
            weight[...], moment[...], second[...], gradient[start:start + count]
        )
        for out, value in zip(outs[3 * i:3 * i + 3], new):
            out[...] = value
        halves.append(new[0].astype(jnp.bfloat16))
        start += count
    query_half, key_half = halves
    query_rows = query_half.shape[0]
    tokens = partial.shape[0]
    for j in range(chips):
        columns = latents[:, :query_rows] if j == 0 else packs[j - 1][grad_rows:, :query_rows]
        product = jnp.dot(columns, query_half, preferred_element_type=jnp.float32)
        if j == 0:
            partial[...] = product
        else:
            gives[j][:tokens, :] = product.astype(jnp.bfloat16)
            gives[j][tokens:, :] = key_half
    gives[0][...] = key_half


def update(total, latents, packs, states):
    chips = len(packs) + 1
    tokens, width = latents.shape
    key_rows = states[3].shape[0]
    *outs, = pl.pallas_call(
        functools.partial(update_kernel, chips),
        out_shape=[jax.ShapeDtypeStruct(x.shape, x.dtype) for x in states]
        + [
            jax.ShapeDtypeStruct((tokens, width), jnp.float32),
            jax.ShapeDtypeStruct((key_rows, width), jnp.bfloat16),
        ]
        + [jax.ShapeDtypeStruct((tokens + key_rows, width), jnp.bfloat16)] * (chips - 1),
        in_specs=[VMEM_SPEC] * (chips + 7),
        out_specs=[VMEM_SPEC] * (chips + 7),
        compiler_params=pltpu.CompilerParams(vmem_limit_bytes=8 << 20),
        cost_estimate=pl.CostEstimate(flops=4 * 10**9, bytes_accessed=10**6, transcendentals=0),
        name="update",
    )(total, latents, *packs, *states)
    return outs[:6], outs[6], outs[7], outs[8:]


def merge_kernel(partial, key_half, *refs):
    *gots, query_sum, pair = refs
    tokens = partial.shape[0] // 2
    key_rows = key_half.shape[0]
    total = partial[...]
    pair[:key_rows, :] = key_half[...]
    for j, got in enumerate(gots):
        total = total + got[:2 * tokens, :].astype(jnp.float32)
        pair[(j + 1) * key_rows:(j + 2) * key_rows, :] = got[2 * tokens:, :]
    query_sum[...] = total[:tokens]
    pair[(len(gots) + 1) * key_rows:, :] = total[tokens:].astype(jnp.bfloat16)


def merge(partial, key_half, gots):
    tokens, width = partial.shape
    rows = (len(gots) + 1) * key_half.shape[0] + tokens // 2
    return pl.pallas_call(
        merge_kernel,
        out_shape=[
            jax.ShapeDtypeStruct((tokens // 2, width), jnp.float32),
            jax.ShapeDtypeStruct((rows, width), jnp.bfloat16),
        ],
        in_specs=[VMEM_SPEC] * (len(gots) + 2),
        out_specs=[VMEM_SPEC] * 2,
        compiler_params=pltpu.CompilerParams(vmem_limit_bytes=2 << 20),
        name="merge",
    )(partial, key_half, *gots)


def attend_kernel(
    rows, shares, whole_out,
    query_sum, pair_own, pair_got, query_rope, new_keys, lengths, value_up, cache, weight,
    *outs,
):
    f32, bf16 = jnp.float32, jnp.bfloat16
    *outs, key_full = outs
    tokens = query_sum.shape[0]
    heads = query_sum.shape[1] // HD
    count = heads * tokens
    chip, core, chips = place()
    key_rows = KL // (2 * chips)
    for j in range(chips):
        for pair, side in ((pair_own, core), (pair_got, 1 - core)):
            at = rows_at(2 * (chip ^ j) + side, key_rows)
            key_full[at, :] = pair[j * key_rows:(j + 1) * key_rows, :]
    head_query = (query_sum[...] + pair_got[KL // 2:, :].astype(f32)).astype(bf16)
    nt = (((1,), (1,)), ((), ()))
    nn = (((1,), (0,)), ((), ()))

    def dot(a, b, dims):
        return lax.dot_general(a, b, dims, preferred_element_type=f32)

    latent_query = jnp.concatenate(
        [
            dot(head_query[:, h * HD:(h + 1) * HD], key_full[:, h * HD:(h + 1) * HD], nt)
            for h in range(heads)
        ]
    ).astype(bf16)
    rope = query_rope[...]
    scale = 1.0 / math.sqrt(HD + R)
    row_of = lax.broadcasted_iota(jnp.int32, (count, 1), 0)
    batch_of, step_of = row_of % rows, (row_of // rows) % STEPS
    scores = jnp.zeros((count, CACHE), f32)
    for b in range(rows):
        here = dot(latent_query, cache[b, :KL, :], nn) + dot(rope, cache[b, KL:, :], nn)
        scores = jnp.where(batch_of == b, here, scores)
    slot = lax.broadcasted_iota(jnp.int32, (count, CACHE), 1)
    scores = jnp.where(slot < row_value(lengths[...], count, rows), scores * scale, -jnp.inf)
    fresh = dot(latent_query, new_keys[:, :KL], nt) + dot(rope, new_keys[:, KL:], nt)
    key_at = lax.broadcasted_iota(jnp.int32, (count, tokens), 1)
    seen = (key_at % rows == batch_of) & (key_at // rows <= step_of)
    fresh = jnp.where(seen, fresh * scale, -jnp.inf)
    highest = jnp.maximum(
        jnp.max(scores, -1, keepdims=True), jnp.max(fresh, -1, keepdims=True)
    )
    scores, fresh = jnp.exp(scores - highest), jnp.exp(fresh - highest)
    denominator = jnp.sum(scores, -1, keepdims=True) + jnp.sum(fresh, -1, keepdims=True)
    probs = (scores / denominator).astype(bf16)
    latent_out = dot((fresh / denominator).astype(bf16), new_keys[:, :KL], nn)
    for b in range(rows):
        mine = jnp.where(batch_of == b, probs, jnp.zeros_like(probs))
        latent_out = latent_out + dot(mine, cache[b, :KL, :], nt)
    latent_out = latent_out.astype(bf16)
    head_values = jnp.concatenate(
        [
            dot(latent_out[h * tokens:(h + 1) * tokens], value_up[:, h * HD:(h + 1) * HD], nn)
            for h in range(heads)
        ],
        1,
    ).astype(bf16)
    into = lax.broadcasted_iota(jnp.int32, (tokens, tokens), 0)
    origin = lax.broadcasted_iota(jnp.int32, (tokens, tokens), 1)
    order = origin == (into % STEPS) * rows + into // STEPS
    order = jnp.where(order, 1.0, 0.0).astype(bf16)
    head_values = dot(order, head_values, nn).astype(bf16)
    if whole_out:
        outs[0][...] = dot(head_values, weight[...], nn)
        return
    share = lax.axis_index("fsdp")
    part = weight.shape[1] // shares
    for j in range(shares):
        columns = pl.ds(pl.multiple_of((share ^ j) * part, 128), part)
        outs[j][...] = dot(head_values, weight[:, columns], nn).astype(outs[j].dtype)


def attend(
    query_sum, pair_own, pair_got, query_rope, new_keys, lengths, value_up, cache, weight
):
    rows = lengths.shape[0]
    tokens, columns = rows * STEPS, weight.shape[1]
    width = query_sum.shape[1]
    shares = lax.axis_size("fsdp")
    part = columns // shares
    whole_out = part % 128 != 0
    if whole_out:
        outs = [jax.ShapeDtypeStruct((tokens, columns), jnp.float32)]
    else:
        outs = [
            jax.ShapeDtypeStruct((tokens, part), jnp.bfloat16 if j else jnp.float32)
            for j in range(shares)
        ]
    outs = pl.pallas_call(
        functools.partial(attend_kernel, rows, shares, whole_out),
        out_shape=outs,
        in_specs=[VMEM_SPEC] * 9,
        out_specs=[VMEM_SPEC] * len(outs),
        scratch_shapes=[pltpu.VMEM((KL, width), jnp.bfloat16)],
        compiler_params=pltpu.CompilerParams(vmem_limit_bytes=24 << 20),
        name="attend",
    )(
        query_sum, pair_own, pair_got, query_rope, new_keys, lengths[None, :],
        value_up, cache, weight,
    )
    if whole_out:
        share = lax.axis_index("fsdp")
        blocks = outs[0].reshape(tokens, shares, part)
        own = block(blocks, share, 1)
        blocks = blocks.astype(jnp.bfloat16)
        return [own] + [block(blocks, share ^ j, 1) for j in range(1, shares)]
    return outs


def per_device(
    query_latent,
    new_entries,
    latent_cache,
    lengths,
    query_up,
    key_up,
    query_moment,
    query_second,
    key_moment,
    key_second,
    query_grads,
    key_grads,
    rope_query,
    value_up,
    output_weight,
):
    _, _, chips = place()
    devices = 2 * chips
    row_count = query_latent.shape[0]
    tokens = row_count * STEPS
    flat_query = query_latent.transpose(1, 0, 2).reshape(tokens, QR)

    query_got = swap(query_grads, ROW_AXES, devices, 1)
    key_got = swap(key_grads, ROW_AXES, devices, 1)
    own, latent_keep, latent_give = own_blocks(query_grads, key_grads, flat_query)
    latent_got = swap(latent_give, ROW_AXES, devices, 1)
    total, columns, packs = pack_sums(own, query_got, key_got, latent_keep, latent_got)
    query_rope, new_keys = rope(
        columns,
        flat_query,
        rope_query,
        new_entries.transpose(1, 0, 2).reshape(tokens, KL + R),
        lengths[None, :],
    )
    packs = [swap(pack, ROW_AXES, devices, 2 * j + 2) for j, pack in enumerate(packs)]

    states = (query_up, query_moment, query_second, key_up, key_moment, key_second)
    states, query_sum, key_half, gives = update(total, columns, packs, states)
    query_weight, query_first, query_square, key_weight, key_first, key_square = states
    gots = [swap(give, ROW_AXES, devices, 2 * j + 2) for j, give in enumerate(gives)]
    query_sum, pair_own = merge(query_sum, key_half, gots)
    pair_got = swap(pair_own, ROW_AXES, devices, 1)
    cache, weight = latent_cache.transpose(0, 2, 1), output_weight
    attended, *give = attend(
        query_sum, pair_own, pair_got, query_rope, new_keys, lengths, value_up, cache, weight
    )
    shares = lax.axis_size("fsdp")
    packs = [swap(pack, "fsdp", shares, j + 1) for j, pack in enumerate(give)]
    for pack in packs:
        attended = attended + pack.astype(jnp.float32)
    attended = attended.astype(jnp.bfloat16).T
    return (query_weight, key_weight, query_first, query_square, key_first, key_square, attended)


def solution(mesh):
    return step(mesh)


def step(mesh):
    return jax.shard_map(
        per_device,
        mesh=mesh,
        in_specs=(
            P(("group", "inner"), None, None),
            P(("group", "inner"), None, None),
            P(("group", "inner"), None, None),
            P(("group", "inner")),
            P(("group", "inner"), "fsdp"),
            P(("group", "inner"), "fsdp"),
            P(("group", "inner"), "fsdp"),
            P(("group", "inner"), "fsdp"),
            P(("group", "inner"), "fsdp"),
            P(("group", "inner"), "fsdp"),
            P(("group", "inner"), "fsdp"),
            P(("group", "inner"), "fsdp"),
            P(None, "fsdp"),
            P(None, "fsdp"),
            P("fsdp", None),
        ),
        out_specs=(
            P(("group", "inner"), "fsdp"),
            P(("group", "inner"), "fsdp"),
            P(("group", "inner"), "fsdp"),
            P(("group", "inner"), "fsdp"),
            P(("group", "inner"), "fsdp"),
            P(("group", "inner"), "fsdp"),
            P("fsdp", ("group", "inner")),
        ),
        check_vma=False,
    )
```

```python
import functools
import math

import jax
import jax.numpy as jnp
from jax import lax
from jax.experimental import pallas as pl
from jax.experimental.pallas import tpu as pltpu
from jax.sharding import PartitionSpec as P


QR = 1536
KL = 512
HD = 128
R = 64
STEPS = 3
CACHE = 512


first_decay = 0.9
second_decay = 0.95
adam_epsilon = 1e-08
weight_decay = 0.1
learn_rate = 0.003
step_count = 10
rope_base = 10000.0


def optimizer_step(weight, moment, second, gradient):
    moment = first_decay * moment + (1.0 - first_decay) * gradient
    second = second_decay * second + (1.0 - second_decay) * gradient * gradient
    first_fix = 1.0 - first_decay**step_count
    second_fix = 1.0 - second_decay**step_count
    update = moment / first_fix / (jnp.sqrt(second / second_fix) + adam_epsilon)
    return (weight - learn_rate * (update + weight_decay * weight), moment, second)


ROW_AXES = ("group", "inner")


def swap(value, axes, count, distance):
    return lax.ppermute(value, axes, [(i, i ^ distance) for i in range(count)])


def block(value, index, axis=0):
    return lax.dynamic_index_in_dim(value, index, axis, keepdims=False)


VMEM_SPEC = pl.BlockSpec(memory_space=pltpu.VMEM)
HBM_SPEC = pl.BlockSpec(memory_space=pltpu.HBM)


def in_hbm(value):
    return pltpu.with_memory_space_constraint(value, pltpu.HBM)


def place():
    me = lax.axis_index(ROW_AXES)
    return me // 2, me % 2, lax.axis_size(ROW_AXES) // 2


def rows_at(index, count):
    return pl.ds(pl.multiple_of(index * count, 16), count)


def own_kernel(query_own, key_own, latents_in, out, keep, give, latents, sems):
    _, core, chips = place()
    fetch = pltpu.make_async_copy(latents_in, latents, sems.at[2 * chips])
    fetch.start()
    copies = []
    for other in range(chips):
        start = 0
        for i, own in enumerate((query_own, key_own)):
            count = own.shape[0] // (2 * chips)
            copies.append(
                pltpu.make_async_copy(
                    own.at[rows_at(2 * other + core, count), :],
                    out.at[other, pl.ds(start, count), :],
                    sems.at[2 * other + i],
                )
            )
            start += count
    for copy in copies:
        copy.start()
    count = query_own.shape[0] // (2 * chips)
    fetch.wait()
    values = latents[...].astype(jnp.float32)
    pad = jnp.zeros((values.shape[0], keep.shape[2] - count), jnp.float32)
    for other in range(chips):
        even, odd = (
            jnp.concatenate(
                [values[:, (2 * other + i) * count:(2 * other + i + 1) * count], pad], 1
            )
            for i in range(2)
        )
        keep[other] = jnp.where(core == 0, even, odd).astype(keep.dtype)
        give[other] = jnp.where(core == 0, odd, even).astype(give.dtype)
    for copy in copies:
        copy.wait()


def own_blocks(query_own, key_own, latents):
    chips = lax.axis_size(ROW_AXES) // 2
    width = query_own.shape[1]
    grad_rows = (query_own.shape[0] + key_own.shape[0]) // (2 * chips)
    return pl.pallas_call(
        own_kernel,
        out_shape=[jax.ShapeDtypeStruct((chips, grad_rows, width), query_own.dtype)]
        + [jax.ShapeDtypeStruct((chips, latents.shape[0], width), latents.dtype)] * 2,
        in_specs=[HBM_SPEC] * 3,
        out_specs=[VMEM_SPEC] * 3,
        scratch_shapes=[
            pltpu.VMEM(latents.shape, latents.dtype),
            pltpu.SemaphoreType.DMA((2 * chips + 1,)),
        ],
        compiler_params=pltpu.CompilerParams(vmem_limit_bytes=2 << 20),
        cost_estimate=pl.CostEstimate(flops=10**9, bytes_accessed=10**6, transcendentals=0),
        name="own",
    )(in_hbm(query_own), in_hbm(key_own), in_hbm(latents))


def pack_kernel(own, query_got, key_got, latent_own, latent_got, *outs):
    chip, core, chips = place()
    total, latent_out, packs = outs[0], outs[1], outs[2:]
    grad_rows = total.shape[0]
    for j in range(chips):
        other = chip ^ j
        start = 0
        for got in (query_got, key_got):
            count = got.shape[0] // (2 * chips)
            both = own[other, start:start + count, :].astype(jnp.float32)
            both = both + got[rows_at(2 * other + core, count), :].astype(jnp.float32)
            if j == 0:
                total[start:start + count, :] = both
            else:
                packs[j - 1][start:start + count, :] = both.astype(jnp.bfloat16)
            start += count
        latents = jnp.concatenate(
            [latent_own[other].astype(jnp.float32), latent_got[other].astype(jnp.float32)]
        ).astype(jnp.bfloat16)
        if j == 0:
            latent_out[...] = latents
        else:
            packs[j - 1][grad_rows:, :] = latents


def pack_sums(own, query_got, key_got, latent_own, latent_got):
    chips, grad_rows, width = own.shape
    tokens = latent_own.shape[1]
    total, latents, *packs = pl.pallas_call(
        pack_kernel,
        out_shape=[
            jax.ShapeDtypeStruct((grad_rows, width), jnp.float32),
            jax.ShapeDtypeStruct((2 * tokens, width), jnp.bfloat16),
        ]
        + [jax.ShapeDtypeStruct((grad_rows + 2 * tokens, width), jnp.bfloat16)] * (chips - 1),
        in_specs=[VMEM_SPEC] * 5,
        out_specs=[VMEM_SPEC] * (chips + 1),
        compiler_params=pltpu.CompilerParams(vmem_limit_bytes=8 << 20),
        cost_estimate=pl.CostEstimate(flops=10**9, bytes_accessed=10**6, transcendentals=0),
        name="pack",
    )(own, query_got, key_got, latent_own, latent_got)
    return total, latents, packs


def row_value(lengths, count, rows):
    token = lax.broadcasted_iota(jnp.int32, (count, rows), 0)
    row = lax.broadcasted_iota(jnp.int32, (count, rows), 1)
    return jnp.sum(jnp.where(token % rows == row, lengths, 0), 1, keepdims=True)


def rope_kernel(after, query, weight, entries, lengths, query_rope, new_keys):
    del after
    tokens, rows = query.shape[0], lengths.shape[1]
    half = R // 2
    step = lax.broadcasted_iota(jnp.int32, (tokens, 1), 0) // rows
    place_of = (row_value(lengths[...], tokens, rows) + step).astype(jnp.float32)
    index = lax.broadcasted_iota(jnp.int32, (tokens, half), 1).astype(jnp.float32)
    angles = place_of * jnp.exp(index * (-math.log(rope_base) / half))
    cosine, sine = jnp.cos(angles), jnp.sin(angles)

    def turn(vectors):
        first, second = vectors[:, :half], vectors[:, half:]
        return jnp.concatenate(
            [first * cosine - second * sine, first * sine + second * cosine], 1
        )

    projected = jnp.dot(query[...], weight[...], preferred_element_type=jnp.float32)
    heads = projected.shape[1] // R
    query_rope[...] = jnp.concatenate(
        [turn(projected[:, h * R:(h + 1) * R]) for h in range(heads)]
    ).astype(jnp.bfloat16)
    new_keys[:, :KL] = entries[:, :KL]
    new_keys[:, KL:] = turn(entries[:, KL:].astype(jnp.float32)).astype(jnp.bfloat16)


def rope(after, query, weight, entries, lengths):
    heads = weight.shape[1] // R
    return pl.pallas_call(
        rope_kernel,
        out_shape=[
            jax.ShapeDtypeStruct((heads * query.shape[0], R), jnp.bfloat16),
            jax.ShapeDtypeStruct(entries.shape, jnp.bfloat16),
        ],
        in_specs=[VMEM_SPEC] * 5,
        out_specs=[VMEM_SPEC] * 2,
        compiler_params=pltpu.CompilerParams(vmem_limit_bytes=4 << 20),
        name="rope",
    )(after, query, weight, entries, lengths)


def update_kernel(chips, *refs):
    total, latents = refs[:2]
    packs, refs = refs[2:chips + 1], refs[chips + 1:]
    states, outs = refs[:6], refs[6:]
    partial, gives = outs[6], outs[7:]
    grad_rows = total.shape[0]
    gradient = total[...]
    for got in packs:
        gradient = gradient + got[:grad_rows, :].astype(jnp.float32)
    start = 0
    halves = []
    for i in range(2):
        weight, moment, second = states[3 * i:3 * i + 3]
        count = weight.shape[0]
        new = optimizer_step(
            weight[...], moment[...], second[...], gradient[start:start + count]
        )
        for out, value in zip(outs[3 * i:3 * i + 3], new):
            out[...] = value
        halves.append(new[0].astype(jnp.bfloat16))
        start += count
    query_half, key_half = halves
    query_rows = query_half.shape[0]
    tokens = partial.shape[0]
    for j in range(chips):
        columns = latents[:, :query_rows] if j == 0 else packs[j - 1][grad_rows:, :query_rows]
        product = jnp.dot(columns, query_half, preferred_element_type=jnp.float32)
        if j == 0:
            partial[...] = product
        else:
            gives[j][:tokens, :] = product.astype(jnp.bfloat16)
            gives[j][tokens:, :] = key_half
    gives[0][...] = key_half


def update(total, latents, packs, states):
    chips = len(packs) + 1
    tokens, width = latents.shape
    key_rows = states[3].shape[0]
    *outs, = pl.pallas_call(
        functools.partial(update_kernel, chips),
        out_shape=[pltpu.VMEM(x.shape, x.dtype) for x in states]
        + [
            jax.ShapeDtypeStruct((tokens, width), jnp.float32),
            jax.ShapeDtypeStruct((key_rows, width), jnp.bfloat16),
        ]
        + [jax.ShapeDtypeStruct((tokens + key_rows, width), jnp.bfloat16)] * (chips - 1),
        in_specs=[VMEM_SPEC] * (chips + 7),
        out_specs=[VMEM_SPEC] * (chips + 7),
        compiler_params=pltpu.CompilerParams(vmem_limit_bytes=8 << 20),
        cost_estimate=pl.CostEstimate(flops=4 * 10**9, bytes_accessed=10**6, transcendentals=0),
        name="update",
    )(total, latents, *packs, *states)
    return outs[:6], outs[6], outs[7], outs[8:]


def merge_kernel(partial, key_half, *refs):
    *gots, query_sum, pair = refs
    tokens = partial.shape[0] // 2
    key_rows = key_half.shape[0]
    total = partial[...]
    pair[:key_rows, :] = key_half[...]
    for j, got in enumerate(gots):
        total = total + got[:2 * tokens, :].astype(jnp.float32)
        pair[(j + 1) * key_rows:(j + 2) * key_rows, :] = got[2 * tokens:, :]
    query_sum[...] = total[:tokens]
    pair[(len(gots) + 1) * key_rows:, :] = total[tokens:].astype(jnp.bfloat16)


def merge(partial, key_half, gots):
    tokens, width = partial.shape
    rows = (len(gots) + 1) * key_half.shape[0] + tokens // 2
    return pl.pallas_call(
        merge_kernel,
        out_shape=[
            jax.ShapeDtypeStruct((tokens // 2, width), jnp.float32),
            jax.ShapeDtypeStruct((rows, width), jnp.bfloat16),
        ],
        in_specs=[VMEM_SPEC] * (len(gots) + 2),
        out_specs=[VMEM_SPEC] * 2,
        compiler_params=pltpu.CompilerParams(vmem_limit_bytes=2 << 20),
        name="merge",
    )(partial, key_half, *gots)


def attend_kernel(
    rows,
    query_sum, pair_own, pair_got, query_rope, new_keys, lengths, value_up, cache,
    out, key_full,
):
    f32, bf16 = jnp.float32, jnp.bfloat16
    tokens = query_sum.shape[0]
    heads = query_sum.shape[1] // HD
    count = heads * tokens
    chip, core, chips = place()
    key_rows = KL // (2 * chips)
    for j in range(chips):
        for pair, side in ((pair_own, core), (pair_got, 1 - core)):
            at = rows_at(2 * (chip ^ j) + side, key_rows)
            key_full[at, :] = pair[j * key_rows:(j + 1) * key_rows, :]
    head_query = (query_sum[...] + pair_got[KL // 2:, :].astype(f32)).astype(bf16)
    nt = (((1,), (1,)), ((), ()))
    nn = (((1,), (0,)), ((), ()))

    def dot(a, b, dims):
        return lax.dot_general(a, b, dims, preferred_element_type=f32)

    latent_query = jnp.concatenate(
        [
            dot(head_query[:, h * HD:(h + 1) * HD], key_full[:, h * HD:(h + 1) * HD], nt)
            for h in range(heads)
        ]
    ).astype(bf16)
    rope = query_rope[...]
    scale = 1.0 / math.sqrt(HD + R)
    row_of = lax.broadcasted_iota(jnp.int32, (count, 1), 0)
    batch_of, step_of = row_of % rows, (row_of // rows) % STEPS
    scores = jnp.zeros((count, CACHE), f32)
    for b in range(rows):
        here = dot(latent_query, cache[b, :KL, :], nn) + dot(rope, cache[b, KL:, :], nn)
        scores = jnp.where(batch_of == b, here, scores)
    slot = lax.broadcasted_iota(jnp.int32, (count, CACHE), 1)
    scores = jnp.where(slot < row_value(lengths[...], count, rows), scores * scale, -jnp.inf)
    fresh = dot(latent_query, new_keys[:, :KL], nt) + dot(rope, new_keys[:, KL:], nt)
    key_at = lax.broadcasted_iota(jnp.int32, (count, tokens), 1)
    seen = (key_at % rows == batch_of) & (key_at // rows <= step_of)
    fresh = jnp.where(seen, fresh * scale, -jnp.inf)
    highest = jnp.maximum(
        jnp.max(scores, -1, keepdims=True), jnp.max(fresh, -1, keepdims=True)
    )
    scores, fresh = jnp.exp(scores - highest), jnp.exp(fresh - highest)
    denominator = jnp.sum(scores, -1, keepdims=True) + jnp.sum(fresh, -1, keepdims=True)
    probs = (scores / denominator).astype(bf16)
    latent_out = dot((fresh / denominator).astype(bf16), new_keys[:, :KL], nn)
    for b in range(rows):
        mine = jnp.where(batch_of == b, probs, jnp.zeros_like(probs))
        latent_out = latent_out + dot(mine, cache[b, :KL, :], nt)
    latent_out = latent_out.astype(bf16)
    head_values = jnp.concatenate(
        [
            dot(latent_out[h * tokens:(h + 1) * tokens], value_up[:, h * HD:(h + 1) * HD], nn)
            for h in range(heads)
        ],
        1,
    ).astype(bf16)
    into = lax.broadcasted_iota(jnp.int32, (tokens, tokens), 0)
    origin = lax.broadcasted_iota(jnp.int32, (tokens, tokens), 1)
    order = origin == (into % STEPS) * rows + into // STEPS
    order = jnp.where(order, 1.0, 0.0).astype(bf16)
    out[...] = dot(order, head_values, nn).astype(bf16)


def attend(query_sum, pair_own, pair_got, query_rope, new_keys, lengths, value_up, cache):
    tokens, width = query_sum.shape
    return pl.pallas_call(
        functools.partial(attend_kernel, lengths.shape[0]),
        out_shape=jax.ShapeDtypeStruct((tokens, width), jnp.bfloat16),
        in_specs=[VMEM_SPEC] * 8,
        out_specs=VMEM_SPEC,
        scratch_shapes=[pltpu.VMEM((KL, width), jnp.bfloat16)],
        compiler_params=pltpu.CompilerParams(vmem_limit_bytes=16 << 20),
        name="attend",
    )(query_sum, pair_own, pair_got, query_rope, new_keys, lengths[None, :], value_up, cache)


def project_kernel(distance, head_values, weight, out):
    part = out.shape[1]
    if part == weight.shape[1]:
        columns = weight[...]
    else:
        share = lax.axis_index("fsdp")
        columns = weight[:, pl.ds(pl.multiple_of((share ^ distance) * part, 128), part)]
    out[...] = jnp.dot(
        head_values[...], columns, preferred_element_type=jnp.float32
    ).astype(out.dtype)


def project(head_values, weight, distance, part, dtype):
    return pl.pallas_call(
        functools.partial(project_kernel, distance),
        out_shape=jax.ShapeDtypeStruct((head_values.shape[0], part), dtype),
        in_specs=[VMEM_SPEC] * 2,
        out_specs=VMEM_SPEC,
        compiler_params=pltpu.CompilerParams(vmem_limit_bytes=8 << 20),
        name="project",
    )(head_values, weight)


def project_all(head_values, weight):
    shares = lax.axis_size("fsdp")
    columns = weight.shape[1]
    part = columns // shares
    if part % 128 == 0:
        return [
            project(head_values, weight, j, part, jnp.bfloat16 if j else jnp.float32)
            for j in range(shares)
        ]
    whole = project(head_values, weight, 0, columns, jnp.float32)
    share = lax.axis_index("fsdp")
    blocks = whole.reshape(-1, shares, part)
    own = block(blocks, share, 1)
    blocks = blocks.astype(jnp.bfloat16)
    return [own] + [block(blocks, share ^ j, 1) for j in range(1, shares)]


def per_device(
    query_latent,
    new_entries,
    latent_cache,
    lengths,
    query_up,
    key_up,
    query_moment,
    query_second,
    key_moment,
    key_second,
    query_grads,
    key_grads,
    rope_query,
    value_up,
    output_weight,
):
    _, _, chips = place()
    devices = 2 * chips
    row_count = query_latent.shape[0]
    tokens = row_count * STEPS
    flat_query = query_latent.transpose(1, 0, 2).reshape(tokens, QR)

    query_got = swap(query_grads, ROW_AXES, devices, 1)
    key_got = swap(key_grads, ROW_AXES, devices, 1)
    own, latent_keep, latent_give = own_blocks(query_grads, key_grads, flat_query)
    latent_got = swap(latent_give, ROW_AXES, devices, 1)
    total, columns, packs = pack_sums(own, query_got, key_got, latent_keep, latent_got)
    query_rope, new_keys = rope(
        columns,
        flat_query,
        rope_query,
        new_entries.transpose(1, 0, 2).reshape(tokens, KL + R),
        lengths[None, :],
    )
    packs = [swap(pack, ROW_AXES, devices, 2 * j + 2) for j, pack in enumerate(packs)]

    states = (query_up, query_moment, query_second, key_up, key_moment, key_second)
    states, query_sum, key_half, gives = update(total, columns, packs, states)
    query_weight, query_first, query_square, key_weight, key_first, key_square = states
    gots = [swap(give, ROW_AXES, devices, 2 * j + 2) for j, give in enumerate(gives)]
    query_sum, pair_own = merge(query_sum, key_half, gots)
    pair_got = swap(pair_own, ROW_AXES, devices, 1)
    head_values = attend(
        query_sum, pair_own, pair_got, query_rope, new_keys, lengths, value_up,
        latent_cache.transpose(0, 2, 1),
    )
    attended, *give = project_all(head_values, output_weight)
    shares = lax.axis_size("fsdp")
    packs = [swap(pack, "fsdp", shares, j + 1) for j, pack in enumerate(give)]
    for pack in packs:
        attended = attended + pack.astype(jnp.float32)
    attended = attended.astype(jnp.bfloat16).T
    return (query_weight, key_weight, query_first, query_square, key_first, key_square, attended)


def solution(mesh):
    return step(mesh)


def step(mesh):
    return jax.shard_map(
        per_device,
        mesh=mesh,
        in_specs=(
            P(("group", "inner"), None, None),
            P(("group", "inner"), None, None),
            P(("group", "inner"), None, None),
            P(("group", "inner")),
            P(("group", "inner"), "fsdp"),
            P(("group", "inner"), "fsdp"),
            P(("group", "inner"), "fsdp"),
            P(("group", "inner"), "fsdp"),
            P(("group", "inner"), "fsdp"),
            P(("group", "inner"), "fsdp"),
            P(("group", "inner"), "fsdp"),
            P(("group", "inner"), "fsdp"),
            P(None, "fsdp"),
            P(None, "fsdp"),
            P("fsdp", None),
        ),
        out_specs=(
            P(("group", "inner"), "fsdp"),
            P(("group", "inner"), "fsdp"),
            P(("group", "inner"), "fsdp"),
            P(("group", "inner"), "fsdp"),
            P(("group", "inner"), "fsdp"),
            P(("group", "inner"), "fsdp"),
            P("fsdp", ("group", "inner")),
        ),
        check_vma=False,
    )
```

```python
import functools
import math

import jax
import jax.numpy as jnp
from jax import lax
from jax.experimental import pallas as pl
from jax.experimental.pallas import tpu as pltpu
from jax.sharding import PartitionSpec as P


QR = 1536
KL = 512
HD = 128
R = 64
STEPS = 3
CACHE = 512


first_decay = 0.9
second_decay = 0.95
adam_epsilon = 1e-08
weight_decay = 0.1
learn_rate = 0.003
step_count = 10
rope_base = 10000.0


def optimizer_step(weight, moment, second, gradient):
    moment = first_decay * moment + (1.0 - first_decay) * gradient
    second = second_decay * second + (1.0 - second_decay) * gradient * gradient
    first_fix = 1.0 - first_decay**step_count
    second_fix = 1.0 - second_decay**step_count
    update = moment / first_fix / (jnp.sqrt(second / second_fix) + adam_epsilon)
    return (weight - learn_rate * (update + weight_decay * weight), moment, second)


ROW_AXES = ("group", "inner")


def swap(value, axes, count, distance):
    return lax.ppermute(value, axes, [(i, i ^ distance) for i in range(count)])


def block(value, index, axis=0):
    return lax.dynamic_index_in_dim(value, index, axis, keepdims=False)


VMEM_SPEC = pl.BlockSpec(memory_space=pltpu.VMEM)
HBM_SPEC = pl.BlockSpec(memory_space=pltpu.HBM)


def in_hbm(value):
    return pltpu.with_memory_space_constraint(value, pltpu.HBM)


def place():
    me = lax.axis_index(ROW_AXES)
    return me // 2, me % 2, lax.axis_size(ROW_AXES) // 2


def rows_at(index, count):
    return pl.ds(pl.multiple_of(index * count, 16), count)


def cut(latents, out, core, chips, count):
    values = latents[...].astype(jnp.float32)
    pad = jnp.zeros((values.shape[0], out.shape[2] - count), jnp.float32)
    for other in range(chips):
        even, odd = (
            values[:, (2 * other + i) * count:(2 * other + i + 1) * count] for i in range(2)
        )
        chosen = jnp.concatenate([jnp.where(core == 0, even, odd), pad], 1)
        out[other] = chosen.astype(out.dtype)


def own_kernel(query_own, key_own, latents_in, out, keep, latents, sems):
    _, core, chips = place()
    fetch = pltpu.make_async_copy(latents_in, latents, sems.at[2 * chips])
    fetch.start()
    copies = []
    for other in range(chips):
        start = 0
        for i, own in enumerate((query_own, key_own)):
            count = own.shape[0] // (2 * chips)
            copies.append(
                pltpu.make_async_copy(
                    own.at[rows_at(2 * other + core, count), :],
                    out.at[other, pl.ds(start, count), :],
                    sems.at[2 * other + i],
                )
            )
            start += count
    for copy in copies:
        copy.start()
    fetch.wait()
    cut(latents, keep, core, chips, query_own.shape[0] // (2 * chips))
    for copy in copies:
        copy.wait()


def own_blocks(query_own, key_own, latents):
    chips = lax.axis_size(ROW_AXES) // 2
    width = query_own.shape[1]
    grad_rows = (query_own.shape[0] + key_own.shape[0]) // (2 * chips)
    return pl.pallas_call(
        own_kernel,
        out_shape=[
            jax.ShapeDtypeStruct((chips, grad_rows, width), query_own.dtype),
            jax.ShapeDtypeStruct((chips, latents.shape[0], width), latents.dtype),
        ],
        in_specs=[HBM_SPEC] * 3,
        out_specs=[VMEM_SPEC] * 2,
        scratch_shapes=[
            pltpu.VMEM(latents.shape, latents.dtype),
            pltpu.SemaphoreType.DMA((2 * chips + 1,)),
        ],
        compiler_params=pltpu.CompilerParams(vmem_limit_bytes=2 << 20),
        cost_estimate=pl.CostEstimate(flops=10**9, bytes_accessed=10**6, transcendentals=0),
        name="own",
    )(in_hbm(query_own), in_hbm(key_own), in_hbm(latents))


def pack_kernel(own, query_got, key_got, latent_own, latents, *outs):
    chip, core, chips = place()
    *outs, latent_got = outs
    total, latent_out, packs = outs[0], outs[1], outs[2:]
    grad_rows = total.shape[0]
    cut(latents, latent_got, core, chips, query_got.shape[0] // (2 * chips))
    for j in range(chips):
        other = chip ^ j
        start = 0
        for got in (query_got, key_got):
            count = got.shape[0] // (2 * chips)
            both = own[other, start:start + count, :].astype(jnp.float32)
            both = both + got[rows_at(2 * other + core, count), :].astype(jnp.float32)
            if j == 0:
                total[start:start + count, :] = both
            else:
                packs[j - 1][start:start + count, :] = both.astype(jnp.bfloat16)
            start += count
        pair = jnp.concatenate(
            [latent_own[other].astype(jnp.float32), latent_got[other].astype(jnp.float32)]
        ).astype(jnp.bfloat16)
        if j == 0:
            latent_out[...] = pair
        else:
            packs[j - 1][grad_rows:, :] = pair


def pack_sums(own, query_got, key_got, latent_own, latents):
    chips, grad_rows, width = own.shape
    tokens = latent_own.shape[1]
    total, columns, *packs = pl.pallas_call(
        pack_kernel,
        out_shape=[
            jax.ShapeDtypeStruct((grad_rows, width), jnp.float32),
            jax.ShapeDtypeStruct((2 * tokens, width), jnp.bfloat16),
        ]
        + [jax.ShapeDtypeStruct((grad_rows + 2 * tokens, width), jnp.bfloat16)] * (chips - 1),
        in_specs=[VMEM_SPEC] * 5,
        out_specs=[VMEM_SPEC] * (chips + 1),
        scratch_shapes=[pltpu.VMEM(latent_own.shape, latent_own.dtype)],
        compiler_params=pltpu.CompilerParams(vmem_limit_bytes=8 << 20),
        cost_estimate=pl.CostEstimate(flops=10**9, bytes_accessed=10**6, transcendentals=0),
        name="pack",
    )(own, query_got, key_got, latent_own, latents)
    return total, columns, packs


def row_value(lengths, count, rows):
    token = lax.broadcasted_iota(jnp.int32, (count, rows), 0)
    row = lax.broadcasted_iota(jnp.int32, (count, rows), 1)
    return jnp.sum(jnp.where(token % rows == row, lengths, 0), 1, keepdims=True)


def rope_kernel(
    after, query, weight, entries, lengths, cache, query_rope, new_keys, scores_out
):
    del after
    tokens, rows = query.shape[0], lengths.shape[1]
    half = R // 2
    step = lax.broadcasted_iota(jnp.int32, (tokens, 1), 0) // rows
    place_of = (row_value(lengths[...], tokens, rows) + step).astype(jnp.float32)
    index = lax.broadcasted_iota(jnp.int32, (tokens, half), 1).astype(jnp.float32)
    angles = place_of * jnp.exp(index * (-math.log(rope_base) / half))
    cosine, sine = jnp.cos(angles), jnp.sin(angles)

    def turn(vectors):
        first, second = vectors[:, :half], vectors[:, half:]
        return jnp.concatenate(
            [first * cosine - second * sine, first * sine + second * cosine], 1
        )

    projected = jnp.dot(query[...], weight[...], preferred_element_type=jnp.float32)
    heads = projected.shape[1] // R
    turned = jnp.concatenate(
        [turn(projected[:, h * R:(h + 1) * R]) for h in range(heads)]
    ).astype(jnp.bfloat16)
    query_rope[...] = turned
    batch_of = lax.broadcasted_iota(jnp.int32, (heads * tokens, 1), 0) % rows
    scores = jnp.zeros(scores_out.shape, jnp.float32)
    for b in range(rows):
        here = jnp.dot(turned, cache[b, KL:, :], preferred_element_type=jnp.float32)
        scores = jnp.where(batch_of == b, here, scores)
    scores_out[...] = scores
    new_keys[:, :KL] = entries[:, :KL]
    new_keys[:, KL:] = turn(entries[:, KL:].astype(jnp.float32)).astype(jnp.bfloat16)


def rope(after, query, weight, entries, lengths, cache):
    heads = weight.shape[1] // R
    return pl.pallas_call(
        rope_kernel,
        out_shape=[
            jax.ShapeDtypeStruct((heads * query.shape[0], R), jnp.bfloat16),
            jax.ShapeDtypeStruct(entries.shape, jnp.bfloat16),
            jax.ShapeDtypeStruct((heads * query.shape[0], CACHE), jnp.float32),
        ],
        in_specs=[VMEM_SPEC] * 6,
        out_specs=[VMEM_SPEC] * 3,
        compiler_params=pltpu.CompilerParams(vmem_limit_bytes=4 << 20),
        name="rope",
    )(after, query, weight, entries, lengths, cache)


def update_kernel(chips, *refs):
    total, latents = refs[:2]
    packs, refs = refs[2:chips + 1], refs[chips + 1:]
    states, outs = refs[:6], refs[6:]
    partial, gives = outs[6], outs[7:]
    grad_rows = total.shape[0]
    gradient = total[...]
    for got in packs:
        gradient = gradient + got[:grad_rows, :].astype(jnp.float32)
    start = 0
    halves = []
    for i in range(2):
        weight, moment, second = states[3 * i:3 * i + 3]
        count = weight.shape[0]
        new = optimizer_step(
            weight[...], moment[...], second[...], gradient[start:start + count]
        )
        for out, value in zip(outs[3 * i:3 * i + 3], new):
            out[...] = value
        halves.append(new[0].astype(jnp.bfloat16))
        start += count
    query_half, key_half = halves
    query_rows = query_half.shape[0]
    tokens = partial.shape[0]
    for j in range(chips):
        columns = latents[:, :query_rows] if j == 0 else packs[j - 1][grad_rows:, :query_rows]
        product = jnp.dot(columns, query_half, preferred_element_type=jnp.float32)
        if j == 0:
            partial[...] = product
        else:
            gives[j][:tokens, :] = product.astype(jnp.bfloat16)
            gives[j][tokens:, :] = key_half
    gives[0][...] = key_half


def update(total, latents, packs, states):
    chips = len(packs) + 1
    tokens, width = latents.shape
    key_rows = states[3].shape[0]
    *outs, = pl.pallas_call(
        functools.partial(update_kernel, chips),
        out_shape=[pltpu.VMEM(x.shape, x.dtype) for x in states]
        + [
            jax.ShapeDtypeStruct((tokens, width), jnp.float32),
            jax.ShapeDtypeStruct((key_rows, width), jnp.bfloat16),
        ]
        + [jax.ShapeDtypeStruct((tokens + key_rows, width), jnp.bfloat16)] * (chips - 1),
        in_specs=[VMEM_SPEC] * (chips + 7),
        out_specs=[VMEM_SPEC] * (chips + 7),
        compiler_params=pltpu.CompilerParams(vmem_limit_bytes=8 << 20),
        cost_estimate=pl.CostEstimate(flops=4 * 10**9, bytes_accessed=10**6, transcendentals=0),
        name="update",
    )(total, latents, *packs, *states)
    return outs[:6], outs[6], outs[7], outs[8:]


def merge_kernel(partial, key_half, *refs):
    *gots, query_sum, pair = refs
    tokens = partial.shape[0] // 2
    key_rows = key_half.shape[0]
    total = partial[...]
    pair[:key_rows, :] = key_half[...]
    for j, got in enumerate(gots):
        total = total + got[:2 * tokens, :].astype(jnp.float32)
        pair[(j + 1) * key_rows:(j + 2) * key_rows, :] = got[2 * tokens:, :]
    query_sum[...] = total[:tokens]
    pair[(len(gots) + 1) * key_rows:, :] = total[tokens:].astype(jnp.bfloat16)


def merge(partial, key_half, gots):
    tokens, width = partial.shape
    rows = (len(gots) + 1) * key_half.shape[0] + tokens // 2
    return pl.pallas_call(
        merge_kernel,
        out_shape=[
            jax.ShapeDtypeStruct((tokens // 2, width), jnp.float32),
            jax.ShapeDtypeStruct((rows, width), jnp.bfloat16),
        ],
        in_specs=[VMEM_SPEC] * (len(gots) + 2),
        out_specs=[VMEM_SPEC] * 2,
        compiler_params=pltpu.CompilerParams(vmem_limit_bytes=2 << 20),
        name="merge",
    )(partial, key_half, *gots)


def attend_kernel(
    rows,
    query_sum, pair_own, pair_got, query_rope, new_keys, rope_scores, lengths, value_up, cache,
    out, key_full,
):
    f32, bf16 = jnp.float32, jnp.bfloat16
    tokens = query_sum.shape[0]
    heads = query_sum.shape[1] // HD
    count = heads * tokens
    chip, core, chips = place()
    key_rows = KL // (2 * chips)
    for j in range(chips):
        for pair, side in ((pair_own, core), (pair_got, 1 - core)):
            at = rows_at(2 * (chip ^ j) + side, key_rows)
            key_full[at, :] = pair[j * key_rows:(j + 1) * key_rows, :]
    head_query = (query_sum[...] + pair_got[KL // 2:, :].astype(f32)).astype(bf16)
    nt = (((1,), (1,)), ((), ()))
    nn = (((1,), (0,)), ((), ()))

    def dot(a, b, dims):
        return lax.dot_general(a, b, dims, preferred_element_type=f32)

    latent_query = jnp.concatenate(
        [
            dot(head_query[:, h * HD:(h + 1) * HD], key_full[:, h * HD:(h + 1) * HD], nt)
            for h in range(heads)
        ]
    ).astype(bf16)
    rope = query_rope[...]
    scale = 1.0 / math.sqrt(HD + R)
    row_of = lax.broadcasted_iota(jnp.int32, (count, 1), 0)
    batch_of, step_of = row_of % rows, (row_of // rows) % STEPS
    scores = jnp.zeros((count, CACHE), f32)
    for b in range(rows):
        here = dot(latent_query, cache[b, :KL, :], nn)
        scores = jnp.where(batch_of == b, here, scores)
    slot = lax.broadcasted_iota(jnp.int32, (count, CACHE), 1)
    scores = jnp.where(slot < row_value(lengths[...], count, rows), (scores + rope_scores[...]) * scale, -jnp.inf)
    fresh = dot(latent_query, new_keys[:, :KL], nt) + dot(rope, new_keys[:, KL:], nt)
    key_at = lax.broadcasted_iota(jnp.int32, (count, tokens), 1)
    seen = (key_at % rows == batch_of) & (key_at // rows <= step_of)
    fresh = jnp.where(seen, fresh * scale, -jnp.inf)
    highest = jnp.maximum(
        jnp.max(scores, -1, keepdims=True), jnp.max(fresh, -1, keepdims=True)
    )
    scores, fresh = jnp.exp(scores - highest), jnp.exp(fresh - highest)
    denominator = jnp.sum(scores, -1, keepdims=True) + jnp.sum(fresh, -1, keepdims=True)
    probs = (scores / denominator).astype(bf16)
    latent_out = dot((fresh / denominator).astype(bf16), new_keys[:, :KL], nn)
    for b in range(rows):
        mine = jnp.where(batch_of == b, probs, jnp.zeros_like(probs))
        latent_out = latent_out + dot(mine, cache[b, :KL, :], nt)
    latent_out = latent_out.astype(bf16)
    head_values = jnp.concatenate(
        [
            dot(latent_out[h * tokens:(h + 1) * tokens], value_up[:, h * HD:(h + 1) * HD], nn)
            for h in range(heads)
        ],
        1,
    ).astype(bf16)
    into = lax.broadcasted_iota(jnp.int32, (tokens, tokens), 0)
    origin = lax.broadcasted_iota(jnp.int32, (tokens, tokens), 1)
    order = origin == (into % STEPS) * rows + into // STEPS
    order = jnp.where(order, 1.0, 0.0).astype(bf16)
    out[...] = dot(order, head_values, nn).astype(bf16)


def attend(
    query_sum, pair_own, pair_got, query_rope, new_keys, rope_scores, lengths, value_up, cache
):
    tokens, width = query_sum.shape
    return pl.pallas_call(
        functools.partial(attend_kernel, lengths.shape[0]),
        out_shape=jax.ShapeDtypeStruct((tokens, width), jnp.bfloat16),
        in_specs=[VMEM_SPEC] * 9,
        out_specs=VMEM_SPEC,
        scratch_shapes=[pltpu.VMEM((KL, width), jnp.bfloat16)],
        compiler_params=pltpu.CompilerParams(vmem_limit_bytes=16 << 20),
        name="attend",
    )(
        query_sum, pair_own, pair_got, query_rope, new_keys, rope_scores, lengths[None, :],
        value_up, cache,
    )


def project_kernel(distance, head_values, weight, out):
    part = out.shape[1]
    if part == weight.shape[1]:
        columns = weight[...]
    else:
        share = lax.axis_index("fsdp")
        columns = weight[:, pl.ds(pl.multiple_of((share ^ distance) * part, 128), part)]
    out[...] = jnp.dot(
        head_values[...], columns, preferred_element_type=jnp.float32
    ).astype(out.dtype)


def project(head_values, weight, distance, part, dtype):
    return pl.pallas_call(
        functools.partial(project_kernel, distance),
        out_shape=jax.ShapeDtypeStruct((head_values.shape[0], part), dtype),
        in_specs=[VMEM_SPEC] * 2,
        out_specs=VMEM_SPEC,
        compiler_params=pltpu.CompilerParams(vmem_limit_bytes=8 << 20),
        name="project",
    )(head_values, weight)


def project_all(head_values, weight):
    shares = lax.axis_size("fsdp")
    columns = weight.shape[1]
    part = columns // shares
    if part % 128 == 0:
        return [
            project(head_values, weight, j, part, jnp.bfloat16 if j else jnp.float32)
            for j in range(shares)
        ]
    whole = project(head_values, weight, 0, columns, jnp.float32)
    share = lax.axis_index("fsdp")
    blocks = whole.reshape(-1, shares, part)
    own = block(blocks, share, 1)
    blocks = blocks.astype(jnp.bfloat16)
    return [own] + [block(blocks, share ^ j, 1) for j in range(1, shares)]


def per_device(
    query_latent,
    new_entries,
    latent_cache,
    lengths,
    query_up,
    key_up,
    query_moment,
    query_second,
    key_moment,
    key_second,
    query_grads,
    key_grads,
    rope_query,
    value_up,
    output_weight,
):
    _, _, chips = place()
    devices = 2 * chips
    row_count = query_latent.shape[0]
    tokens = row_count * STEPS
    flat_query = query_latent.transpose(1, 0, 2).reshape(tokens, QR)

    query_got = swap(query_grads, ROW_AXES, devices, 1)
    key_got = swap(key_grads, ROW_AXES, devices, 1)
    latent_got = swap(flat_query, ROW_AXES, devices, 1)
    own, latent_own = own_blocks(query_grads, key_grads, flat_query)
    total, columns, packs = pack_sums(own, query_got, key_got, latent_own, latent_got)
    cache = latent_cache.transpose(0, 2, 1)
    query_rope, new_keys, rope_scores = rope(
        columns,
        flat_query,
        rope_query,
        new_entries.transpose(1, 0, 2).reshape(tokens, KL + R),
        lengths[None, :],
        cache,
    )
    packs = [swap(pack, ROW_AXES, devices, 2 * j + 2) for j, pack in enumerate(packs)]

    states = (query_up, query_moment, query_second, key_up, key_moment, key_second)
    states, query_sum, key_half, gives = update(total, columns, packs, states)
    query_weight, query_first, query_square, key_weight, key_first, key_square = states
    gots = [swap(give, ROW_AXES, devices, 2 * j + 2) for j, give in enumerate(gives)]
    query_sum, pair_own = merge(query_sum, key_half, gots)
    pair_got = swap(pair_own, ROW_AXES, devices, 1)
    head_values = attend(
        query_sum, pair_own, pair_got, query_rope, new_keys, rope_scores, lengths, value_up,
        cache,
    )
    attended, *give = project_all(head_values, output_weight)
    shares = lax.axis_size("fsdp")
    packs = [swap(pack, "fsdp", shares, j + 1) for j, pack in enumerate(give)]
    for pack in packs:
        attended = attended + pack.astype(jnp.float32)
    attended = attended.astype(jnp.bfloat16).T
    return (query_weight, key_weight, query_first, query_square, key_first, key_square, attended)


def solution(mesh):
    return step(mesh)


def step(mesh):
    return jax.shard_map(
        per_device,
        mesh=mesh,
        in_specs=(
            P(("group", "inner"), None, None),
            P(("group", "inner"), None, None),
            P(("group", "inner"), None, None),
            P(("group", "inner")),
            P(("group", "inner"), "fsdp"),
            P(("group", "inner"), "fsdp"),
            P(("group", "inner"), "fsdp"),
            P(("group", "inner"), "fsdp"),
            P(("group", "inner"), "fsdp"),
            P(("group", "inner"), "fsdp"),
            P(("group", "inner"), "fsdp"),
            P(("group", "inner"), "fsdp"),
            P(None, "fsdp"),
            P(None, "fsdp"),
            P("fsdp", None),
        ),
        out_specs=(
            P(("group", "inner"), "fsdp"),
            P(("group", "inner"), "fsdp"),
            P(("group", "inner"), "fsdp"),
            P(("group", "inner"), "fsdp"),
            P(("group", "inner"), "fsdp"),
            P(("group", "inner"), "fsdp"),
            P("fsdp", ("group", "inner")),
        ),
        check_vma=False,
    )
```

```python
import functools
import math

import jax
import jax.numpy as jnp
from jax import lax
from jax.experimental import pallas as pl
from jax.experimental.pallas import tpu as pltpu
from jax.sharding import PartitionSpec as P


QR = 1536
KL = 512
HD = 128
R = 64
STEPS = 3
CACHE = 512


first_decay = 0.9
second_decay = 0.95
adam_epsilon = 1e-08
weight_decay = 0.1
learn_rate = 0.003
step_count = 10
rope_base = 10000.0


def optimizer_step(weight, moment, second, gradient):
    moment = first_decay * moment + (1.0 - first_decay) * gradient
    second = second_decay * second + (1.0 - second_decay) * gradient * gradient
    first_fix = 1.0 - first_decay**step_count
    second_fix = 1.0 - second_decay**step_count
    update = moment / first_fix / (jnp.sqrt(second / second_fix) + adam_epsilon)
    return (weight - learn_rate * (update + weight_decay * weight), moment, second)


ROW_AXES = ("group", "inner")


def swap(value, axes, count, distance):
    return lax.ppermute(value, axes, [(i, i ^ distance) for i in range(count)])


def block(value, index, axis=0):
    return lax.dynamic_index_in_dim(value, index, axis, keepdims=False)


VMEM_SPEC = pl.BlockSpec(memory_space=pltpu.VMEM)
HBM_SPEC = pl.BlockSpec(memory_space=pltpu.HBM)


def in_hbm(value):
    return pltpu.with_memory_space_constraint(value, pltpu.HBM)


def place():
    me = lax.axis_index(ROW_AXES)
    return me // 2, me % 2, lax.axis_size(ROW_AXES) // 2


def rows_at(index, count):
    return pl.ds(pl.multiple_of(index * count, 16), count)


def cut(latents, out, core, chips, count):
    values = latents[...].astype(jnp.float32)
    pad = jnp.zeros((values.shape[0], out.shape[2] - count), jnp.float32)
    for other in range(chips):
        even, odd = (
            values[:, (2 * other + i) * count:(2 * other + i + 1) * count] for i in range(2)
        )
        chosen = jnp.concatenate([jnp.where(core == 0, even, odd), pad], 1)
        out[other] = chosen.astype(out.dtype)


def own_kernel(query_own, key_own, latents_in, out, keep, latents, sems):
    _, core, chips = place()
    fetch = pltpu.make_async_copy(latents_in, latents, sems.at[2 * chips])
    fetch.start()
    copies = []
    for other in range(chips):
        start = 0
        for i, own in enumerate((query_own, key_own)):
            count = own.shape[0] // (2 * chips)
            copies.append(
                pltpu.make_async_copy(
                    own.at[rows_at(2 * other + core, count), :],
                    out.at[other, pl.ds(start, count), :],
                    sems.at[2 * other + i],
                )
            )
            start += count
    for copy in copies:
        copy.start()
    fetch.wait()
    cut(latents, keep, core, chips, query_own.shape[0] // (2 * chips))
    for copy in copies:
        copy.wait()


def own_blocks(query_own, key_own, latents):
    chips = lax.axis_size(ROW_AXES) // 2
    width = query_own.shape[1]
    grad_rows = (query_own.shape[0] + key_own.shape[0]) // (2 * chips)
    return pl.pallas_call(
        own_kernel,
        out_shape=[
            jax.ShapeDtypeStruct((chips, grad_rows, width), query_own.dtype),
            jax.ShapeDtypeStruct((chips, latents.shape[0], width), latents.dtype),
        ],
        in_specs=[HBM_SPEC] * 3,
        out_specs=[VMEM_SPEC] * 2,
        scratch_shapes=[
            pltpu.VMEM(latents.shape, latents.dtype),
            pltpu.SemaphoreType.DMA((2 * chips + 1,)),
        ],
        compiler_params=pltpu.CompilerParams(vmem_limit_bytes=2 << 20),
        cost_estimate=pl.CostEstimate(flops=10**9, bytes_accessed=10**6, transcendentals=0),
        name="own",
    )(in_hbm(query_own), in_hbm(key_own), in_hbm(latents))


def pack_kernel(own, query_got, key_got, latent_own, latents, *outs):
    chip, core, chips = place()
    *outs, latent_got = outs
    total, latent_out, packs = outs[0], outs[1], outs[2:]
    grad_rows = total.shape[0]
    cut(latents, latent_got, core, chips, query_got.shape[0] // (2 * chips))
    for j in range(chips):
        other = chip ^ j
        start = 0
        for got in (query_got, key_got):
            count = got.shape[0] // (2 * chips)
            both = own[other, start:start + count, :].astype(jnp.float32)
            both = both + got[rows_at(2 * other + core, count), :].astype(jnp.float32)
            if j == 0:
                total[start:start + count, :] = both
            else:
                packs[j - 1][start:start + count, :] = both.astype(jnp.bfloat16)
            start += count
        pair = jnp.concatenate(
            [latent_own[other].astype(jnp.float32), latent_got[other].astype(jnp.float32)]
        ).astype(jnp.bfloat16)
        if j == 0:
            latent_out[...] = pair
        else:
            packs[j - 1][grad_rows:, :] = pair


def pack_sums(own, query_got, key_got, latent_own, latents):
    chips, grad_rows, width = own.shape
    tokens = latent_own.shape[1]
    total, columns, *packs = pl.pallas_call(
        pack_kernel,
        out_shape=[
            jax.ShapeDtypeStruct((grad_rows, width), jnp.float32),
            jax.ShapeDtypeStruct((2 * tokens, width), jnp.bfloat16),
        ]
        + [jax.ShapeDtypeStruct((grad_rows + 2 * tokens, width), jnp.bfloat16)] * (chips - 1),
        in_specs=[VMEM_SPEC] * 5,
        out_specs=[VMEM_SPEC] * (chips + 1),
        scratch_shapes=[pltpu.VMEM(latent_own.shape, latent_own.dtype)],
        compiler_params=pltpu.CompilerParams(vmem_limit_bytes=8 << 20),
        cost_estimate=pl.CostEstimate(flops=10**9, bytes_accessed=10**6, transcendentals=0),
        name="pack",
    )(own, query_got, key_got, latent_own, latents)
    return total, columns, packs


def row_value(lengths, count, rows):
    token = lax.broadcasted_iota(jnp.int32, (count, rows), 0)
    row = lax.broadcasted_iota(jnp.int32, (count, rows), 1)
    return jnp.sum(jnp.where(token % rows == row, lengths, 0), 1, keepdims=True)


def rope_kernel(
    after, query, weight, entries, lengths, cache, query_rope, new_keys, scores_out
):
    del after
    tokens, rows = query.shape[0], lengths.shape[1]
    half = R // 2
    step = lax.broadcasted_iota(jnp.int32, (tokens, 1), 0) // rows
    place_of = (row_value(lengths[...], tokens, rows) + step).astype(jnp.float32)
    index = lax.broadcasted_iota(jnp.int32, (tokens, half), 1).astype(jnp.float32)
    angles = place_of * jnp.exp(index * (-math.log(rope_base) / half))
    cosine, sine = jnp.cos(angles), jnp.sin(angles)

    def turn(vectors):
        first, second = vectors[:, :half], vectors[:, half:]
        return jnp.concatenate(
            [first * cosine - second * sine, first * sine + second * cosine], 1
        )

    projected = jnp.dot(query[...], weight[...], preferred_element_type=jnp.float32)
    heads = projected.shape[1] // R
    turned = jnp.concatenate(
        [turn(projected[:, h * R:(h + 1) * R]) for h in range(heads)]
    ).astype(jnp.bfloat16)
    query_rope[...] = turned
    batch_of = lax.broadcasted_iota(jnp.int32, (heads * tokens, 1), 0) % rows
    scores = jnp.zeros(scores_out.shape, jnp.float32)
    for b in range(rows):
        here = jnp.dot(turned, cache[b, KL:, :], preferred_element_type=jnp.float32)
        scores = jnp.where(batch_of == b, here, scores)
    scores_out[...] = scores
    new_keys[:, :KL] = entries[:, :KL]
    new_keys[:, KL:] = turn(entries[:, KL:].astype(jnp.float32)).astype(jnp.bfloat16)


def rope(after, query, weight, entries, lengths, cache):
    heads = weight.shape[1] // R
    return pl.pallas_call(
        rope_kernel,
        out_shape=[
            jax.ShapeDtypeStruct((heads * query.shape[0], R), jnp.bfloat16),
            jax.ShapeDtypeStruct(entries.shape, jnp.bfloat16),
            jax.ShapeDtypeStruct((heads * query.shape[0], CACHE), jnp.float32),
        ],
        in_specs=[VMEM_SPEC] * 6,
        out_specs=[VMEM_SPEC] * 3,
        compiler_params=pltpu.CompilerParams(vmem_limit_bytes=4 << 20),
        name="rope",
    )(after, query, weight, entries, lengths, cache)


def flip_kernel(after, cache, out, done):
    del after
    for b in range(cache.shape[0]):
        out[b] = cache[b, :KL, :].T
    done[...] = jnp.zeros_like(done)


def flip(after, cache):
    return pl.pallas_call(
        flip_kernel,
        out_shape=[
            jax.ShapeDtypeStruct((cache.shape[0], CACHE, KL), cache.dtype),
            jax.ShapeDtypeStruct((8, 128), jnp.float32),
        ],
        in_specs=[VMEM_SPEC] * 2,
        out_specs=[VMEM_SPEC] * 2,
        compiler_params=pltpu.CompilerParams(vmem_limit_bytes=4 << 20),
        cost_estimate=pl.CostEstimate(flops=4 * 10**9, bytes_accessed=10**6, transcendentals=0),
        name="flip",
    )(after, cache)


def update_kernel(chips, done, *refs):
    del done
    total, latents = refs[:2]
    packs, refs = refs[2:chips + 1], refs[chips + 1:]
    states, outs = refs[:6], refs[6:]
    partial, gives = outs[6], outs[7:]
    grad_rows = total.shape[0]
    gradient = total[...]
    for got in packs:
        gradient = gradient + got[:grad_rows, :].astype(jnp.float32)
    start = 0
    halves = []
    for i in range(2):
        weight, moment, second = states[3 * i:3 * i + 3]
        count = weight.shape[0]
        new = optimizer_step(
            weight[...], moment[...], second[...], gradient[start:start + count]
        )
        for out, value in zip(outs[3 * i:3 * i + 3], new):
            out[...] = value
        halves.append(new[0].astype(jnp.bfloat16))
        start += count
    query_half, key_half = halves
    query_rows = query_half.shape[0]
    tokens = partial.shape[0]
    for j in range(chips):
        columns = latents[:, :query_rows] if j == 0 else packs[j - 1][grad_rows:, :query_rows]
        product = jnp.dot(columns, query_half, preferred_element_type=jnp.float32)
        if j == 0:
            partial[...] = product
        else:
            gives[j][:tokens, :] = product.astype(jnp.bfloat16)
            gives[j][tokens:, :] = key_half
    gives[0][...] = key_half


def update(done, total, latents, packs, states):
    chips = len(packs) + 1
    tokens, width = latents.shape
    key_rows = states[3].shape[0]
    *outs, = pl.pallas_call(
        functools.partial(update_kernel, chips),
        out_shape=[pltpu.VMEM(x.shape, x.dtype) for x in states]
        + [
            jax.ShapeDtypeStruct((tokens, width), jnp.float32),
            jax.ShapeDtypeStruct((key_rows, width), jnp.bfloat16),
        ]
        + [jax.ShapeDtypeStruct((tokens + key_rows, width), jnp.bfloat16)] * (chips - 1),
        in_specs=[VMEM_SPEC] * (chips + 8),
        out_specs=[VMEM_SPEC] * (chips + 7),
        compiler_params=pltpu.CompilerParams(vmem_limit_bytes=8 << 20),
        cost_estimate=pl.CostEstimate(flops=4 * 10**9, bytes_accessed=10**6, transcendentals=0),
        name="update",
    )(done, total, latents, *packs, *states)
    return outs[:6], outs[6], outs[7], outs[8:]


def merge_kernel(partial, key_half, *refs):
    *gots, query_sum, pair = refs
    tokens = partial.shape[0] // 2
    key_rows = key_half.shape[0]
    total = partial[...]
    pair[:key_rows, :] = key_half[...]
    for j, got in enumerate(gots):
        total = total + got[:2 * tokens, :].astype(jnp.float32)
        pair[(j + 1) * key_rows:(j + 2) * key_rows, :] = got[2 * tokens:, :]
    query_sum[...] = total[:tokens]
    pair[(len(gots) + 1) * key_rows:, :] = total[tokens:].astype(jnp.bfloat16)


def merge(partial, key_half, gots):
    tokens, width = partial.shape
    rows = (len(gots) + 1) * key_half.shape[0] + tokens // 2
    return pl.pallas_call(
        merge_kernel,
        out_shape=[
            jax.ShapeDtypeStruct((tokens // 2, width), jnp.float32),
            jax.ShapeDtypeStruct((rows, width), jnp.bfloat16),
        ],
        in_specs=[VMEM_SPEC] * (len(gots) + 2),
        out_specs=[VMEM_SPEC] * 2,
        compiler_params=pltpu.CompilerParams(vmem_limit_bytes=2 << 20),
        name="merge",
    )(partial, key_half, *gots)


def attend_kernel(
    rows,
    query_sum, pair_own, pair_got, query_rope, new_keys, rope_scores, lengths, value_up, cache, flipped,
    out, key_full,
):
    f32, bf16 = jnp.float32, jnp.bfloat16
    tokens = query_sum.shape[0]
    heads = query_sum.shape[1] // HD
    count = heads * tokens
    chip, core, chips = place()
    key_rows = KL // (2 * chips)
    for j in range(chips):
        for pair, side in ((pair_own, core), (pair_got, 1 - core)):
            at = rows_at(2 * (chip ^ j) + side, key_rows)
            key_full[at, :] = pair[j * key_rows:(j + 1) * key_rows, :]
    head_query = (query_sum[...] + pair_got[KL // 2:, :].astype(f32)).astype(bf16)
    nt = (((1,), (1,)), ((), ()))
    nn = (((1,), (0,)), ((), ()))

    def dot(a, b, dims):
        return lax.dot_general(a, b, dims, preferred_element_type=f32)

    latent_query = jnp.concatenate(
        [
            dot(head_query[:, h * HD:(h + 1) * HD], key_full[:, h * HD:(h + 1) * HD], nt)
            for h in range(heads)
        ]
    ).astype(bf16)
    rope = query_rope[...]
    scale = 1.0 / math.sqrt(HD + R)
    row_of = lax.broadcasted_iota(jnp.int32, (count, 1), 0)
    batch_of, step_of = row_of % rows, (row_of // rows) % STEPS
    scores = jnp.zeros((count, CACHE), f32)
    for b in range(rows):
        here = dot(latent_query, cache[b, :KL, :], nn)
        scores = jnp.where(batch_of == b, here, scores)
    slot = lax.broadcasted_iota(jnp.int32, (count, CACHE), 1)
    scores = jnp.where(slot < row_value(lengths[...], count, rows), (scores + rope_scores[...]) * scale, -jnp.inf)
    fresh = dot(latent_query, new_keys[:, :KL], nt) + dot(rope, new_keys[:, KL:], nt)
    key_at = lax.broadcasted_iota(jnp.int32, (count, tokens), 1)
    seen = (key_at % rows == batch_of) & (key_at // rows <= step_of)
    fresh = jnp.where(seen, fresh * scale, -jnp.inf)
    highest = jnp.maximum(
        jnp.max(scores, -1, keepdims=True), jnp.max(fresh, -1, keepdims=True)
    )
    scores, fresh = jnp.exp(scores - highest), jnp.exp(fresh - highest)
    denominator = jnp.sum(scores, -1, keepdims=True) + jnp.sum(fresh, -1, keepdims=True)
    probs = (scores / denominator).astype(bf16)
    latent_out = dot((fresh / denominator).astype(bf16), new_keys[:, :KL], nn)
    for b in range(rows):
        mine = jnp.where(batch_of == b, probs, jnp.zeros_like(probs))
        latent_out = latent_out + dot(mine, flipped[b], nn)
    latent_out = latent_out.astype(bf16)
    head_values = jnp.concatenate(
        [
            dot(latent_out[h * tokens:(h + 1) * tokens], value_up[:, h * HD:(h + 1) * HD], nn)
            for h in range(heads)
        ],
        1,
    ).astype(bf16)
    into = lax.broadcasted_iota(jnp.int32, (tokens, tokens), 0)
    origin = lax.broadcasted_iota(jnp.int32, (tokens, tokens), 1)
    order = origin == (into % STEPS) * rows + into // STEPS
    order = jnp.where(order, 1.0, 0.0).astype(bf16)
    out[...] = dot(order, head_values, nn).astype(bf16)


def attend(
    query_sum, pair_own, pair_got, query_rope, new_keys, rope_scores, lengths, value_up, cache,
    flipped,
):
    tokens, width = query_sum.shape
    return pl.pallas_call(
        functools.partial(attend_kernel, lengths.shape[0]),
        out_shape=jax.ShapeDtypeStruct((tokens, width), jnp.bfloat16),
        in_specs=[VMEM_SPEC] * 10,
        out_specs=VMEM_SPEC,
        scratch_shapes=[pltpu.VMEM((KL, width), jnp.bfloat16)],
        compiler_params=pltpu.CompilerParams(vmem_limit_bytes=16 << 20),
        name="attend",
    )(
        query_sum, pair_own, pair_got, query_rope, new_keys, rope_scores, lengths[None, :],
        value_up, cache, flipped,
    )


def project_kernel(distance, head_values, weight, out):
    part = out.shape[1]
    if part == weight.shape[1]:
        columns = weight[...]
    else:
        share = lax.axis_index("fsdp")
        columns = weight[:, pl.ds(pl.multiple_of((share ^ distance) * part, 128), part)]
    out[...] = jnp.dot(
        head_values[...], columns, preferred_element_type=jnp.float32
    ).astype(out.dtype)


def project(head_values, weight, distance, part, dtype):
    return pl.pallas_call(
        functools.partial(project_kernel, distance),
        out_shape=jax.ShapeDtypeStruct((head_values.shape[0], part), dtype),
        in_specs=[VMEM_SPEC] * 2,
        out_specs=VMEM_SPEC,
        compiler_params=pltpu.CompilerParams(vmem_limit_bytes=8 << 20),
        name="project",
    )(head_values, weight)


def project_all(head_values, weight):
    shares = lax.axis_size("fsdp")
    columns = weight.shape[1]
    part = columns // shares
    if part % 128 == 0:
        return [
            project(head_values, weight, j, part, jnp.bfloat16 if j else jnp.float32)
            for j in range(shares)
        ]
    whole = project(head_values, weight, 0, columns, jnp.float32)
    share = lax.axis_index("fsdp")
    blocks = whole.reshape(-1, shares, part)
    own = block(blocks, share, 1)
    blocks = blocks.astype(jnp.bfloat16)
    return [own] + [block(blocks, share ^ j, 1) for j in range(1, shares)]


def per_device(
    query_latent,
    new_entries,
    latent_cache,
    lengths,
    query_up,
    key_up,
    query_moment,
    query_second,
    key_moment,
    key_second,
    query_grads,
    key_grads,
    rope_query,
    value_up,
    output_weight,
):
    _, _, chips = place()
    devices = 2 * chips
    row_count = query_latent.shape[0]
    tokens = row_count * STEPS
    flat_query = query_latent.transpose(1, 0, 2).reshape(tokens, QR)

    query_got = swap(query_grads, ROW_AXES, devices, 1)
    key_got = swap(key_grads, ROW_AXES, devices, 1)
    latent_got = swap(flat_query, ROW_AXES, devices, 1)
    own, latent_own = own_blocks(query_grads, key_grads, flat_query)
    total, columns, packs = pack_sums(own, query_got, key_got, latent_own, latent_got)
    cache = latent_cache.transpose(0, 2, 1)
    flipped, done = flip(columns, cache)
    query_rope, new_keys, rope_scores = rope(
        columns,
        flat_query,
        rope_query,
        new_entries.transpose(1, 0, 2).reshape(tokens, KL + R),
        lengths[None, :],
        cache,
    )
    packs = [swap(pack, ROW_AXES, devices, 2 * j + 2) for j, pack in enumerate(packs)]

    states = (query_up, query_moment, query_second, key_up, key_moment, key_second)
    states, query_sum, key_half, gives = update(done, total, columns, packs, states)
    query_weight, query_first, query_square, key_weight, key_first, key_square = states
    gots = [swap(give, ROW_AXES, devices, 2 * j + 2) for j, give in enumerate(gives)]
    query_sum, pair_own = merge(query_sum, key_half, gots)
    pair_got = swap(pair_own, ROW_AXES, devices, 1)
    head_values = attend(
        query_sum, pair_own, pair_got, query_rope, new_keys, rope_scores, lengths, value_up,
        cache, flipped,
    )
    attended, *give = project_all(head_values, output_weight)
    shares = lax.axis_size("fsdp")
    packs = [swap(pack, "fsdp", shares, j + 1) for j, pack in enumerate(give)]
    for pack in packs:
        attended = attended + pack.astype(jnp.float32)
    attended = attended.astype(jnp.bfloat16).T
    return (query_weight, key_weight, query_first, query_square, key_first, key_square, attended)


def solution(mesh):
    return step(mesh)


def step(mesh):
    return jax.shard_map(
        per_device,
        mesh=mesh,
        in_specs=(
            P(("group", "inner"), None, None),
            P(("group", "inner"), None, None),
            P(("group", "inner"), None, None),
            P(("group", "inner")),
            P(("group", "inner"), "fsdp"),
            P(("group", "inner"), "fsdp"),
            P(("group", "inner"), "fsdp"),
            P(("group", "inner"), "fsdp"),
            P(("group", "inner"), "fsdp"),
            P(("group", "inner"), "fsdp"),
            P(("group", "inner"), "fsdp"),
            P(("group", "inner"), "fsdp"),
            P(None, "fsdp"),
            P(None, "fsdp"),
            P("fsdp", None),
        ),
        out_specs=(
            P(("group", "inner"), "fsdp"),
            P(("group", "inner"), "fsdp"),
            P(("group", "inner"), "fsdp"),
            P(("group", "inner"), "fsdp"),
            P(("group", "inner"), "fsdp"),
            P(("group", "inner"), "fsdp"),
            P("fsdp", ("group", "inner")),
        ),
        check_vma=False,
    )
```

```python
import functools
import math

import jax
import jax.numpy as jnp
from jax import lax
from jax.experimental import pallas as pl
from jax.experimental.pallas import tpu as pltpu
from jax.sharding import PartitionSpec as P


QR = 1536
KL = 512
HD = 128
R = 64
STEPS = 3
CACHE = 512


first_decay = 0.9
second_decay = 0.95
adam_epsilon = 1e-08
weight_decay = 0.1
learn_rate = 0.003
step_count = 10
rope_base = 10000.0


def optimizer_step(weight, moment, second, gradient):
    moment = first_decay * moment + (1.0 - first_decay) * gradient
    second = second_decay * second + (1.0 - second_decay) * gradient * gradient
    first_fix = 1.0 - first_decay**step_count
    second_fix = 1.0 - second_decay**step_count
    update = moment / first_fix / (jnp.sqrt(second / second_fix) + adam_epsilon)
    return (weight - learn_rate * (update + weight_decay * weight), moment, second)


ROW_AXES = ("group", "inner")


def swap(value, axes, count, distance):
    return lax.ppermute(value, axes, [(i, i ^ distance) for i in range(count)])


def block(value, index, axis=0):
    return lax.dynamic_index_in_dim(value, index, axis, keepdims=False)


VMEM_SPEC = pl.BlockSpec(memory_space=pltpu.VMEM)
HBM_SPEC = pl.BlockSpec(memory_space=pltpu.HBM)


def in_hbm(value):
    return pltpu.with_memory_space_constraint(value, pltpu.HBM)


def place():
    me = lax.axis_index(ROW_AXES)
    return me // 2, me % 2, lax.axis_size(ROW_AXES) // 2


def rows_at(index, count):
    return pl.ds(pl.multiple_of(index * count, 16), count)


def cut(latents, out, core, chips, count):
    values = latents[...].astype(jnp.float32)
    pad = jnp.zeros((values.shape[0], out.shape[2] - count), jnp.float32)
    for other in range(chips):
        even, odd = (
            values[:, (2 * other + i) * count:(2 * other + i + 1) * count] for i in range(2)
        )
        chosen = jnp.concatenate([jnp.where(core == 0, even, odd), pad], 1)
        out[other] = chosen.astype(out.dtype)


def own_kernel(query_own, key_own, latents_in, out, keep, latents, sems):
    _, core, chips = place()
    fetch = pltpu.make_async_copy(latents_in, latents, sems.at[2 * chips])
    fetch.start()
    copies = []
    for other in range(chips):
        start = 0
        for i, own in enumerate((query_own, key_own)):
            count = own.shape[0] // (2 * chips)
            copies.append(
                pltpu.make_async_copy(
                    own.at[rows_at(2 * other + core, count), :],
                    out.at[other, pl.ds(start, count), :],
                    sems.at[2 * other + i],
                )
            )
            start += count
    for copy in copies:
        copy.start()
    fetch.wait()
    cut(latents, keep, core, chips, query_own.shape[0] // (2 * chips))
    for copy in copies:
        copy.wait()


def own_blocks(query_own, key_own, latents):
    chips = lax.axis_size(ROW_AXES) // 2
    width = query_own.shape[1]
    grad_rows = (query_own.shape[0] + key_own.shape[0]) // (2 * chips)
    return pl.pallas_call(
        own_kernel,
        out_shape=[
            jax.ShapeDtypeStruct((chips, grad_rows, width), query_own.dtype),
            jax.ShapeDtypeStruct((chips, latents.shape[0], width), latents.dtype),
        ],
        in_specs=[HBM_SPEC] * 3,
        out_specs=[VMEM_SPEC] * 2,
        scratch_shapes=[
            pltpu.VMEM(latents.shape, latents.dtype),
            pltpu.SemaphoreType.DMA((2 * chips + 1,)),
        ],
        compiler_params=pltpu.CompilerParams(vmem_limit_bytes=2 << 20),
        cost_estimate=pl.CostEstimate(flops=10**9, bytes_accessed=10**6, transcendentals=0),
        name="own",
    )(in_hbm(query_own), in_hbm(key_own), in_hbm(latents))


def pack_kernel(own, query_got, key_got, latent_own, latents, *outs):
    chip, core, chips = place()
    *outs, latent_got = outs
    total, latent_out, packs = outs[0], outs[1], outs[2:]
    grad_rows = total.shape[0]
    cut(latents, latent_got, core, chips, query_got.shape[0] // (2 * chips))
    for j in range(chips):
        other = chip ^ j
        start = 0
        for got in (query_got, key_got):
            count = got.shape[0] // (2 * chips)
            both = own[other, start:start + count, :].astype(jnp.float32)
            both = both + got[rows_at(2 * other + core, count), :].astype(jnp.float32)
            if j == 0:
                total[start:start + count, :] = both
            else:
                packs[j - 1][start:start + count, :] = both.astype(jnp.bfloat16)
            start += count
        pair = jnp.concatenate(
            [latent_own[other].astype(jnp.float32), latent_got[other].astype(jnp.float32)]
        ).astype(jnp.bfloat16)
        if j == 0:
            latent_out[...] = pair
        else:
            packs[j - 1][grad_rows:, :] = pair


def pack_sums(own, query_got, key_got, latent_own, latents):
    chips, grad_rows, width = own.shape
    tokens = latent_own.shape[1]
    total, columns, *packs = pl.pallas_call(
        pack_kernel,
        out_shape=[
            jax.ShapeDtypeStruct((grad_rows, width), jnp.float32),
            jax.ShapeDtypeStruct((2 * tokens, width), jnp.bfloat16),
        ]
        + [jax.ShapeDtypeStruct((grad_rows + 2 * tokens, width), jnp.bfloat16)] * (chips - 1),
        in_specs=[VMEM_SPEC] * 5,
        out_specs=[VMEM_SPEC] * (chips + 1),
        scratch_shapes=[pltpu.VMEM(latent_own.shape, latent_own.dtype)],
        compiler_params=pltpu.CompilerParams(vmem_limit_bytes=8 << 20),
        cost_estimate=pl.CostEstimate(flops=10**9, bytes_accessed=10**6, transcendentals=0),
        name="pack",
    )(own, query_got, key_got, latent_own, latents)
    return total, columns, packs


def row_value(lengths, count, rows):
    token = lax.broadcasted_iota(jnp.int32, (count, rows), 0)
    row = lax.broadcasted_iota(jnp.int32, (count, rows), 1)
    return jnp.sum(jnp.where(token % rows == row, lengths, 0), 1, keepdims=True)


def rope_kernel(
    after, query, weight, entries, lengths, cache, query_rope, new_keys, scores_out
):
    del after
    tokens, rows = query.shape[0], lengths.shape[1]
    half = R // 2
    step = lax.broadcasted_iota(jnp.int32, (tokens, 1), 0) // rows
    place_of = (row_value(lengths[...], tokens, rows) + step).astype(jnp.float32)
    index = lax.broadcasted_iota(jnp.int32, (tokens, half), 1).astype(jnp.float32)
    angles = place_of * jnp.exp(index * (-math.log(rope_base) / half))
    cosine, sine = jnp.cos(angles), jnp.sin(angles)

    def turn(vectors):
        first, second = vectors[:, :half], vectors[:, half:]
        return jnp.concatenate(
            [first * cosine - second * sine, first * sine + second * cosine], 1
        )

    projected = jnp.dot(query[...], weight[...], preferred_element_type=jnp.float32)
    heads = projected.shape[1] // R
    turned = jnp.concatenate(
        [turn(projected[:, h * R:(h + 1) * R]) for h in range(heads)]
    ).astype(jnp.bfloat16)
    query_rope[...] = turned
    batch_of = lax.broadcasted_iota(jnp.int32, (heads * tokens, 1), 0) % rows
    scores = jnp.zeros(scores_out.shape, jnp.float32)
    for b in range(rows):
        here = jnp.dot(turned, cache[b, KL:, :], preferred_element_type=jnp.float32)
        scores = jnp.where(batch_of == b, here, scores)
    scores_out[...] = scores
    new_keys[:, :KL] = entries[:, :KL]
    new_keys[:, KL:] = turn(entries[:, KL:].astype(jnp.float32)).astype(jnp.bfloat16)


def rope(after, query, weight, entries, lengths, cache):
    heads = weight.shape[1] // R
    return pl.pallas_call(
        rope_kernel,
        out_shape=[
            jax.ShapeDtypeStruct((heads * query.shape[0], R), jnp.bfloat16),
            jax.ShapeDtypeStruct(entries.shape, jnp.bfloat16),
            jax.ShapeDtypeStruct((heads * query.shape[0], CACHE), jnp.float32),
        ],
        in_specs=[VMEM_SPEC] * 6,
        out_specs=[VMEM_SPEC] * 3,
        compiler_params=pltpu.CompilerParams(vmem_limit_bytes=4 << 20),
        name="rope",
    )(after, query, weight, entries, lengths, cache)


def flip_kernel(after, cache, out, done):
    del after
    for b in range(cache.shape[0]):
        out[b] = cache[b, :KL, :].T
    done[...] = jnp.zeros_like(done)


def flip(after, cache):
    return pl.pallas_call(
        flip_kernel,
        out_shape=[
            jax.ShapeDtypeStruct((cache.shape[0], CACHE, KL), cache.dtype),
            jax.ShapeDtypeStruct((8, 128), jnp.float32),
        ],
        in_specs=[VMEM_SPEC] * 2,
        out_specs=[VMEM_SPEC] * 2,
        compiler_params=pltpu.CompilerParams(vmem_limit_bytes=4 << 20),
        cost_estimate=pl.CostEstimate(flops=4 * 10**9, bytes_accessed=10**6, transcendentals=0),
        name="flip",
    )(after, cache)


def update_kernel(chips, done, *refs):
    del done
    total, latents = refs[:2]
    packs, refs = refs[2:chips + 1], refs[chips + 1:]
    states, outs = refs[:6], refs[6:]
    partial, gives = outs[6], outs[7:]
    grad_rows = total.shape[0]
    gradient = total[...]
    for got in packs:
        gradient = gradient + got[:grad_rows, :].astype(jnp.float32)
    start = 0
    halves = []
    for i in range(2):
        weight, moment, second = states[3 * i:3 * i + 3]
        count = weight.shape[0]
        new = optimizer_step(
            weight[...], moment[...], second[...], gradient[start:start + count]
        )
        for out, value in zip(outs[3 * i:3 * i + 3], new):
            out[...] = value
        halves.append(new[0].astype(jnp.bfloat16))
        start += count
    query_half, key_half = halves
    query_rows = query_half.shape[0]
    tokens = partial.shape[0]
    for j in range(chips):
        columns = latents[:, :query_rows] if j == 0 else packs[j - 1][grad_rows:, :query_rows]
        product = jnp.dot(columns, query_half, preferred_element_type=jnp.float32)
        if j == 0:
            partial[...] = product
        else:
            gives[j][:tokens, :] = product.astype(jnp.bfloat16)
            gives[j][tokens:, :] = key_half
    gives[0][...] = key_half


def update(done, total, latents, packs, states):
    chips = len(packs) + 1
    tokens, width = latents.shape
    key_rows = states[3].shape[0]
    *outs, = pl.pallas_call(
        functools.partial(update_kernel, chips),
        out_shape=[pltpu.VMEM(x.shape, x.dtype) for x in states]
        + [
            jax.ShapeDtypeStruct((tokens, width), jnp.float32),
            jax.ShapeDtypeStruct((key_rows, width), jnp.bfloat16),
        ]
        + [jax.ShapeDtypeStruct((tokens + key_rows, width), jnp.bfloat16)] * (chips - 1),
        in_specs=[VMEM_SPEC] * (chips + 8),
        out_specs=[VMEM_SPEC] * (chips + 7),
        compiler_params=pltpu.CompilerParams(vmem_limit_bytes=8 << 20),
        cost_estimate=pl.CostEstimate(flops=4 * 10**9, bytes_accessed=10**6, transcendentals=0),
        name="update",
    )(done, total, latents, *packs, *states)
    return outs[:6], outs[6], outs[7], outs[8:]


def merge_kernel(partial, key_half, *refs):
    *gots, query_sum, pair = refs
    tokens = partial.shape[0] // 2
    key_rows = key_half.shape[0]
    total = partial[...]
    pair[:key_rows, :] = key_half[...]
    for j, got in enumerate(gots):
        total = total + got[:2 * tokens, :].astype(jnp.float32)
        pair[(j + 1) * key_rows:(j + 2) * key_rows, :] = got[2 * tokens:, :]
    query_sum[...] = total[:tokens]
    pair[(len(gots) + 1) * key_rows:, :] = total[tokens:].astype(jnp.bfloat16)


def merge(partial, key_half, gots):
    tokens, width = partial.shape
    rows = (len(gots) + 1) * key_half.shape[0] + tokens // 2
    return pl.pallas_call(
        merge_kernel,
        out_shape=[
            jax.ShapeDtypeStruct((tokens // 2, width), jnp.float32),
            jax.ShapeDtypeStruct((rows, width), jnp.bfloat16),
        ],
        in_specs=[VMEM_SPEC] * (len(gots) + 2),
        out_specs=[VMEM_SPEC] * 2,
        compiler_params=pltpu.CompilerParams(vmem_limit_bytes=2 << 20),
        name="merge",
    )(partial, key_half, *gots)


def attend_kernel(
    rows,
    query_sum, pair_own, pair_got, query_rope, new_keys, rope_scores, lengths, value_up, cache, flipped,
    out, key_full,
):
    f32, bf16 = jnp.float32, jnp.bfloat16
    tokens = query_sum.shape[0]
    heads = query_sum.shape[1] // HD
    count = heads * tokens
    chip, core, chips = place()
    key_rows = KL // (2 * chips)
    for j in range(chips):
        for pair, side in ((pair_own, core), (pair_got, 1 - core)):
            at = rows_at(2 * (chip ^ j) + side, key_rows)
            key_full[at, :] = pair[j * key_rows:(j + 1) * key_rows, :]
    head_query = (query_sum[...] + pair_got[KL // 2:, :].astype(f32)).astype(bf16)
    nt = (((1,), (1,)), ((), ()))
    nn = (((1,), (0,)), ((), ()))

    def dot(a, b, dims):
        return lax.dot_general(a, b, dims, preferred_element_type=f32)

    latent_query = jnp.concatenate(
        [
            dot(head_query[:, h * HD:(h + 1) * HD], key_full[:, h * HD:(h + 1) * HD], nt)
            for h in range(heads)
        ]
    ).astype(bf16)
    rope = query_rope[...]
    scale = 1.0 / math.sqrt(HD + R)
    row_of = lax.broadcasted_iota(jnp.int32, (count, 1), 0)
    batch_of, step_of = row_of % rows, (row_of // rows) % STEPS
    scores = jnp.zeros((count, CACHE), f32)
    for b in range(rows):
        here = dot(latent_query, cache[b, :KL, :], nn)
        scores = jnp.where(batch_of == b, here, scores)
    slot = lax.broadcasted_iota(jnp.int32, (count, CACHE), 1)
    scores = jnp.where(slot < row_value(lengths[...], count, rows), (scores + rope_scores[...]) * scale, -jnp.inf)
    fresh = dot(latent_query, new_keys[:, :KL], nt) + dot(rope, new_keys[:, KL:], nt)
    key_at = lax.broadcasted_iota(jnp.int32, (count, tokens), 1)
    seen = (key_at % rows == batch_of) & (key_at // rows <= step_of)
    fresh = jnp.where(seen, fresh * scale, -jnp.inf)
    highest = jnp.maximum(
        jnp.max(scores, -1, keepdims=True), jnp.max(fresh, -1, keepdims=True)
    )
    scores, fresh = jnp.exp(scores - highest), jnp.exp(fresh - highest)
    denominator = jnp.sum(scores, -1, keepdims=True) + jnp.sum(fresh, -1, keepdims=True)
    inverse = 1.0 / denominator
    probs = (scores * inverse).astype(bf16)
    latent_out = dot((fresh * inverse).astype(bf16), new_keys[:, :KL], nn)
    for b in range(rows):
        mine = jnp.where(batch_of == b, probs, jnp.zeros_like(probs))
        latent_out = latent_out + dot(mine, flipped[b], nn)
    latent_out = latent_out.astype(bf16)
    head_values = jnp.concatenate(
        [
            dot(latent_out[h * tokens:(h + 1) * tokens], value_up[:, h * HD:(h + 1) * HD], nn)
            for h in range(heads)
        ],
        1,
    ).astype(bf16)
    into = lax.broadcasted_iota(jnp.int32, (tokens, tokens), 0)
    origin = lax.broadcasted_iota(jnp.int32, (tokens, tokens), 1)
    order = origin == (into % STEPS) * rows + into // STEPS
    order = jnp.where(order, 1.0, 0.0).astype(bf16)
    out[...] = dot(order, head_values, nn).astype(bf16)


def attend(
    query_sum, pair_own, pair_got, query_rope, new_keys, rope_scores, lengths, value_up, cache,
    flipped,
):
    tokens, width = query_sum.shape
    return pl.pallas_call(
        functools.partial(attend_kernel, lengths.shape[0]),
        out_shape=jax.ShapeDtypeStruct((tokens, width), jnp.bfloat16),
        in_specs=[VMEM_SPEC] * 10,
        out_specs=VMEM_SPEC,
        scratch_shapes=[pltpu.VMEM((KL, width), jnp.bfloat16)],
        compiler_params=pltpu.CompilerParams(vmem_limit_bytes=16 << 20),
        name="attend",
    )(
        query_sum, pair_own, pair_got, query_rope, new_keys, rope_scores, lengths[None, :],
        value_up, cache, flipped,
    )


def project_kernel(distance, head_values, weight, out):
    part = out.shape[1]
    if part == weight.shape[1]:
        columns = weight[...]
    else:
        share = lax.axis_index("fsdp")
        columns = weight[:, pl.ds(pl.multiple_of((share ^ distance) * part, 128), part)]
    out[...] = jnp.dot(
        head_values[...], columns, preferred_element_type=jnp.float32
    ).astype(out.dtype)


def project(head_values, weight, distance, part, dtype):
    return pl.pallas_call(
        functools.partial(project_kernel, distance),
        out_shape=jax.ShapeDtypeStruct((head_values.shape[0], part), dtype),
        in_specs=[VMEM_SPEC] * 2,
        out_specs=VMEM_SPEC,
        compiler_params=pltpu.CompilerParams(vmem_limit_bytes=8 << 20),
        name="project",
    )(head_values, weight)


def project_all(head_values, weight):
    shares = lax.axis_size("fsdp")
    columns = weight.shape[1]
    part = columns // shares
    if part % 128 == 0:
        return [
            project(head_values, weight, j, part, jnp.bfloat16 if j else jnp.float32)
            for j in range(shares)
        ]
    whole = project(head_values, weight, 0, columns, jnp.float32)
    share = lax.axis_index("fsdp")
    blocks = whole.reshape(-1, shares, part)
    own = block(blocks, share, 1)
    blocks = blocks.astype(jnp.bfloat16)
    return [own] + [block(blocks, share ^ j, 1) for j in range(1, shares)]


def per_device(
    query_latent,
    new_entries,
    latent_cache,
    lengths,
    query_up,
    key_up,
    query_moment,
    query_second,
    key_moment,
    key_second,
    query_grads,
    key_grads,
    rope_query,
    value_up,
    output_weight,
):
    _, _, chips = place()
    devices = 2 * chips
    row_count = query_latent.shape[0]
    tokens = row_count * STEPS
    flat_query = query_latent.transpose(1, 0, 2).reshape(tokens, QR)

    query_got = swap(query_grads, ROW_AXES, devices, 1)
    key_got = swap(key_grads, ROW_AXES, devices, 1)
    latent_got = swap(flat_query, ROW_AXES, devices, 1)
    own, latent_own = own_blocks(query_grads, key_grads, flat_query)
    total, columns, packs = pack_sums(own, query_got, key_got, latent_own, latent_got)
    cache = latent_cache.transpose(0, 2, 1)
    flipped, done = flip(columns, cache)
    query_rope, new_keys, rope_scores = rope(
        columns,
        flat_query,
        rope_query,
        new_entries.transpose(1, 0, 2).reshape(tokens, KL + R),
        lengths[None, :],
        cache,
    )
    packs = [swap(pack, ROW_AXES, devices, 2 * j + 2) for j, pack in enumerate(packs)]

    states = (query_up, query_moment, query_second, key_up, key_moment, key_second)
    states, query_sum, key_half, gives = update(done, total, columns, packs, states)
    query_weight, query_first, query_square, key_weight, key_first, key_square = states
    gots = [swap(give, ROW_AXES, devices, 2 * j + 2) for j, give in enumerate(gives)]
    query_sum, pair_own = merge(query_sum, key_half, gots)
    pair_got = swap(pair_own, ROW_AXES, devices, 1)
    head_values = attend(
        query_sum, pair_own, pair_got, query_rope, new_keys, rope_scores, lengths, value_up,
        cache, flipped,
    )
    attended, *give = project_all(head_values, output_weight)
    shares = lax.axis_size("fsdp")
    packs = [swap(pack, "fsdp", shares, j + 1) for j, pack in enumerate(give)]
    for pack in packs:
        attended = attended + pack.astype(jnp.float32)
    attended = attended.astype(jnp.bfloat16).T
    return (query_weight, key_weight, query_first, query_square, key_first, key_square, attended)


def solution(mesh):
    return step(mesh)


def step(mesh):
    return jax.shard_map(
        per_device,
        mesh=mesh,
        in_specs=(
            P(("group", "inner"), None, None),
            P(("group", "inner"), None, None),
            P(("group", "inner"), None, None),
            P(("group", "inner")),
            P(("group", "inner"), "fsdp"),
            P(("group", "inner"), "fsdp"),
            P(("group", "inner"), "fsdp"),
            P(("group", "inner"), "fsdp"),
            P(("group", "inner"), "fsdp"),
            P(("group", "inner"), "fsdp"),
            P(("group", "inner"), "fsdp"),
            P(("group", "inner"), "fsdp"),
            P(None, "fsdp"),
            P(None, "fsdp"),
            P("fsdp", None),
        ),
        out_specs=(
            P(("group", "inner"), "fsdp"),
            P(("group", "inner"), "fsdp"),
            P(("group", "inner"), "fsdp"),
            P(("group", "inner"), "fsdp"),
            P(("group", "inner"), "fsdp"),
            P(("group", "inner"), "fsdp"),
            P("fsdp", ("group", "inner")),
        ),
        check_vma=False,
    )
```
